16 devices in a mesh: dp: 2 (over y, z), tp: 8 (over x, core).
Axes of the slice: x: 4, y: 2, z: 1, core: 2. Of those that a mesh axis runs over, the one named last changes fastest.
The devices are a block of a 4x4x8 slice.
Arguments:
- x: bfloat16 [4096, 2048], P('dp'), parts along dimension 0
- dy: bfloat16 [4096, 2048], P('dp'), parts along dimension 0
- gate: bfloat16 [4096, 8192], P('dp', 'tp'), parts along dimension 0
- up: bfloat16 [4096, 8192], P('dp', 'tp'), parts along dimension 0
- w_gate: bfloat16 [2048, 8192], P(None, 'tp')
- w_up: bfloat16 [2048, 8192], P(None, 'tp')
- w_down: bfloat16 [8192, 2048], P('tp')
Outputs:
- output 1: bfloat16 [4096, 2048], P('dp'), parts along dimension 0
- output 2: bfloat16 [4096, 8192], P('dp', 'tp'), parts along dimension 0
- output 3: bfloat16 [4096, 8192], P('dp', 'tp'), parts along dimension 0
- output 4: bfloat16 [16384, 2048], P(('dp', 'tp')), parts along dimension 0
There are 2 independent parts. The reference program is written for one: setup_inputs(seed, part) draws one part's arguments, and reference() takes and returns one part's arrays. A program takes and returns all parts, laid end to end along the dimension named above; an argument that names none is the same for every part.
All inputs are finite; a program needn't handle non-finite values.
Results may differ from the reference program's by a relative error of at most 0.012.
Values are sent between devices in bfloat16 or wider.
A program may use at most 768 MiB of HBM per device.

```python
import jax
import jax.numpy as jnp

ROWS = 2048
D = 2048
FF = 8192


def act(gate, up):
    return jax.nn.silu(gate) * up


def setup_inputs(seed: int = 0, part: int = 0) -> dict:
    kx, ky, ka, kb, kg, ku, kd = jax.random.split(jax.random.key(seed), 7)
    kx, ky, ka, kb = (jax.random.fold_in(k, part) for k in (kx, ky, ka, kb))
    drawn = {
        "x": jax.random.normal(kx, (ROWS, D), jnp.float32),
        "dy": jax.random.normal(ky, (ROWS, D), jnp.float32),
        "gate": jax.random.normal(ka, (ROWS, FF), jnp.float32),
        "up": jax.random.normal(kb, (ROWS, FF), jnp.float32),
        "w_gate": jax.random.normal(kg, (D, FF), jnp.float32) * D**-0.5,
        "w_up": jax.random.normal(ku, (D, FF), jnp.float32) * D**-0.5,
        "w_down": jax.random.normal(kd, (FF, D), jnp.float32) * FF**-0.5,
    }
    return {k: v.astype(jnp.bfloat16) for k, v in drawn.items()}


def reference(x, dy, gate, up, w_gate, w_up, w_down):
    hidden, back = jax.vjp(act, gate.astype(jnp.float32), up.astype(jnp.float32))
    d_hidden = jnp.dot(dy, w_down.T, preferred_element_type=jnp.float32)
    d_gate, d_up = (g.astype(jnp.bfloat16) for g in back(d_hidden))
    dx = jnp.dot(d_gate, w_gate.T, preferred_element_type=jnp.float32) + jnp.dot(d_up, w_up.T, preferred_element_type=jnp.float32)
    dw_gate = jnp.dot(x.T, d_gate, preferred_element_type=jnp.float32)
    dw_up = jnp.dot(x.T, d_up, preferred_element_type=jnp.float32)
    dw_down = jnp.dot(hidden.astype(jnp.bfloat16).T, dy, preferred_element_type=jnp.float32)
    return tuple(g.astype(jnp.bfloat16) for g in (dx, dw_gate, dw_up, dw_down))
```

```python
import functools

import jax
import jax.numpy as jnp
from jax import lax
from jax.experimental import pallas as pl
from jax.experimental.pallas import tpu as pltpu
from jax.sharding import PartitionSpec as P


BF16, F32 = jnp.bfloat16, jnp.float32
CONTRACT_LAST = (((1,), (1,)), ((), ()))
CONTRACT_FIRST = (((0,), (0,)), ((), ()))
CORES = 2
CHUNKS = (256, 512, 512, 512, 256)
FAR, RIGHT, LEFT, OWN = range(4)
PAIRS = ((FAR, RIGHT), (LEFT, OWN))


def dot_tb(a, b):
    return lax.dot_general(a, b, CONTRACT_LAST, preferred_element_type=F32)


def reduce_kernel(
    n, dy_hbm, gate_hbm, up_hbm, wg_hbm, wu_hbm, wd_hbm, dg_hbm, du_hbm, hid_hbm, red_hbm,
    wcat, wd, dy, d, hid, psend, precv, fsend, frecv, nsend, nrecv, dep, own, red,
    wcat_sem, wd_sem, in_sem, out_sem, red_sem, p_ssem, p_rsem, f_ssem, f_rsem, n_ssem, n_rsem,
):
    rows, width = dy.shape
    ff = wd.shape[0]
    piece = width // n
    chips = n // CORES
    steps = len(CHUNKS)

    t = lax.axis_index("tp")
    chip, core = lax.div(t, CORES), lax.rem(t, CORES)
    partner = t + 1 - 2 * core
    right, left = lax.rem(t + CORES, n), lax.rem(t + n - CORES, n)
    owner = [lax.rem(chip + hop, chips) for hop in (2, 1, chips - 1, 0)]

    def load_rows(i, r0, m):
        rr = pl.ds(r0, m)
        return [
            pltpu.make_async_copy(dy_hbm.at[rr], dy.at[rr], in_sem.at[i, 0]),
            pltpu.make_async_copy(gate_hbm.at[rr], d.at[rr, pl.ds(0, ff)], in_sem.at[i, 1]),
            pltpu.make_async_copy(up_hbm.at[rr], d.at[rr, pl.ds(ff, ff)], in_sem.at[i, 2]),
        ]

    blocks = ff // piece

    def load_wd(b):
        rr = pl.ds(b * piece, piece)
        return pltpu.make_async_copy(wd_hbm.at[rr], wd.at[rr], wd_sem.at[b])

    def load_wcat(half, j):
        whose = lax.rem(core + 1 + half, CORES)
        src = pl.ds(pl.multiple_of((whose * chips + owner[j]) * piece, piece), piece)
        dst = pl.ds((half * chips + j) * piece, piece)
        return [
            pltpu.make_async_copy(w.at[src], wcat.at[dst, pl.ds(k * ff, ff)], wcat_sem.at[half, j, k])
            for k, w in enumerate((wg_hbm, wu_hbm))
        ]

    def load_half(half):
        for j in range(4):
            for c in load_wcat(half, j):
                c.start()

    starts = [sum(CHUNKS[:i]) for i in range(steps)]
    for c in load_rows(0, starts[0], CHUNKS[0]):
        c.start()
    for b in range(blocks):
        load_wd(b).start()

    barrier = pltpu.get_barrier_semaphore()
    for other in (partner, left, right):
        pl.semaphore_signal(barrier, inc=1, device_id={"tp": other})

    def column(j):
        return pl.ds(j * piece, piece)

    def to_partner(i, r0, m, j):
        rr = pl.ds(r0, m)
        return pltpu.make_async_remote_copy(
            psend.at[rr, column(j)], precv.at[rr, column(j)], p_ssem.at[i, j], p_rsem.at[i, j], device_id={"tp": partner}
        )

    def far_copy(i, r0, m, side):
        rr = pl.ds(r0 + side * (m // 2), m // 2)
        return pltpu.make_async_remote_copy(
            fsend.at[rr], frecv.at[rr], f_ssem.at[i, side], f_rsem.at[i, side], device_id={"tp": (right, left)[side]}
        )

    def near_copy(i, r0, m, side, half):
        rr = pl.ds(r0 + half * (m // 2), m // 2)
        return pltpu.make_async_remote_copy(
            nsend.at[side, rr], nrecv.at[side, rr], n_ssem.at[i, side, half], n_rsem.at[i, side, half],
            device_id={"tp": (right, left)[side]},
        )

    def write_out(i, r0, m):
        rr = pl.ds(r0, m)
        return [
            pltpu.make_async_copy(d.at[rr, pl.ds(0, ff)], dg_hbm.at[rr], out_sem.at[i, 0]),
            pltpu.make_async_copy(d.at[rr, pl.ds(ff, ff)], du_hbm.at[rr], out_sem.at[i, 1]),
            pltpu.make_async_copy(hid.at[rr], hid_hbm.at[rr], out_sem.at[i, 2]),
        ]

    def write_red(i, r0, m):
        rr = pl.ds(r0, m)
        return pltpu.make_async_copy(red.at[rr], red_hbm.at[rr], red_sem.at[i])

    def grads(i, r0, m, first=False, midway=None):
        rr = pl.ds(r0, m)
        with jax.named_scope("w_in"):
            for c in load_rows(i, r0, m):
                c.wait()
        if first:
            load_half(0)
            with jax.named_scope("w_wd"):
                for b in range(blocks):
                    load_wd(b).wait()
            load_half(1)
        for b in range(blocks):
            if midway and b == blocks // 2:
                midway()
            cg, cu = column(b), pl.ds(ff + b * piece, piece)
            dh = dot_tb(dy[rr, :], wd[column(b), :])
            g, u = d[rr, cg].astype(F32), d[rr, cu].astype(F32)
            s = jax.nn.sigmoid(g)
            silu = g * s
            hid[rr, cg] = (silu * u).astype(BF16)
            d[rr, cg] = (dh * u * (s + silu * (1.0 - s))).astype(BF16)
            d[rr, cu] = (dh * silu).astype(BF16)
        for c in write_out(i, r0, m):
            c.start()

    def exchange(i, r0, m, first=False):
        rr = pl.ds(r0, m)
        if first:
            for c in load_rows(1, starts[1], CHUNKS[1]):
                c.start()
            with jax.named_scope("w_bar"):
                pl.semaphore_wait(barrier, 3)
        for group in PAIRS:
            if first:
                with jax.named_scope("w_c0"):
                    for j in group:
                        for c in load_wcat(0, j):
                            c.wait()
            for j in group:
                psend[rr, column(j)] = dot_tb(d[rr, :], wcat[column(j), :]).astype(BF16)
            for j in group:
                to_partner(i, r0, m, j).start()

    def terms(i, r0, m, first=False):
        h = m // 2
        rr, top, bottom = pl.ds(r0, m), pl.ds(r0, h), pl.ds(r0 + h, h)
        for group in PAIRS:
            for j in group:
                if first:
                    with jax.named_scope("w_c1"):
                        for c in load_wcat(1, j):
                            c.wait()
                with jax.named_scope("w_p"):
                    to_partner(i, r0, m, j).wait_recv()
            for j in group:
                v = dot_tb(d[rr, :], wcat[column(chips + j), :]) + precv[rr, column(j)].astype(F32)
                if j == FAR:
                    fsend[rr, :] = v.astype(BF16)
                elif j == RIGHT:
                    nsend[0, bottom, :] = v[h:].astype(BF16)
                    dep[0, pl.ds(0, h), :] = v[:h]
                elif j == LEFT:
                    nsend[1, top, :] = v[:h].astype(BF16)
                    dep[1, pl.ds(0, h), :] = v[h:]
                else:
                    own[lax.rem(i, 2), pl.ds(0, m), :] = v
            if FAR in group:
                for side in range(2):
                    far_copy(i, r0, m, side).start()

    def direct(i, r0, m):
        near_copy(i, r0, m, 0, 1).start()
        near_copy(i, r0, m, 1, 0).start()

    def forward(i, r0, m):
        h = m // 2
        for side in range(2):
            rr = pl.ds(r0 + side * h, h)
            with jax.named_scope('w_f'):
                far_copy(i, r0, m, side).wait_recv()
            nsend[side, rr, :] = (dep[side, pl.ds(0, h), :] + frecv[rr, :].astype(F32)).astype(BF16)
            near_copy(i, r0, m, side, side).start()

    def finish(i, r0, m):
        rr = pl.ds(r0, m)
        for side in range(2):
            for half in range(2):
                with jax.named_scope('w_n'):
                    near_copy(i, r0, m, side, half).wait_recv()
        red[rr, :] = (own[lax.rem(i, 2), pl.ds(0, m), :] + nrecv[0, rr, :].astype(F32) + nrecv[1, rr, :].astype(F32)).astype(BF16)
        write_red(i, r0, m).start()

    def step(i, r0, m, next_m, last_m, first=False):
        with jax.named_scope("terms"):
            terms(i, r0, m, first)
        if first:
            for k in range(2, steps):
                for c in load_rows(k, starts[k], CHUNKS[k]):
                    c.start()
        if next_m:
            with jax.named_scope("grads"):
                grads(i + 1, r0 + m, next_m, midway=lambda: direct(i, r0, m))
        else:
            with jax.named_scope("w_s"):
                for side in range(2):
                    far_copy(i, r0, m, side).wait_send()
            direct(i, r0, m)
        with jax.named_scope("forward"):
            forward(i, r0, m)
        if next_m:
            with jax.named_scope("exchange"):
                exchange(i + 1, r0 + m, next_m)
        if last_m:
            with jax.named_scope("finish"):
                finish(i - 1, r0 - last_m, last_m)

    with jax.named_scope("grads"):
        grads(0, 0, CHUNKS[0], True)
    with jax.named_scope("exchange"):
        exchange(0, 0, CHUNKS[0], True)
    i = 0
    while i < steps:
        key = (CHUNKS[i], CHUNKS[i + 1] if i + 1 < steps else 0, CHUNKS[i - 1] if i else 0)
        same = 1
        while 0 < i and i + same + 1 < steps and (CHUNKS[i + same], CHUNKS[i + same + 1], CHUNKS[i + same - 1]) == key:
            same += 1
        if same == 1:
            step(i, starts[i], *key, first=i == 0)
        else:
            base, r0, m = i, starts[i], CHUNKS[i]

            @pl.loop(0, same)
            def _(k):
                step(base + k, pl.multiple_of(r0 + k * m, piece), *key)

        i += same
    finish(steps - 1, starts[-1], CHUNKS[-1])

    for i, (r0, m) in enumerate(zip(starts, CHUNKS)):
        for c in write_out(i, r0, m):
            c.wait()
        write_red(i, r0, m).wait()
        for j in range(4):
            to_partner(i, r0, m, j).wait_send()
        for side in range(2):
            if i + 1 < steps:
                far_copy(i, r0, m, side).wait_send()
            for half in range(2):
                near_copy(i, r0, m, side, half).wait_send()


def reduce_terms(n, dy, gate, up, wg, wu, wd):
    rows, width = dy.shape
    ff = gate.shape[1]
    piece = width // n
    steps = len(CHUNKS)
    big = max(CHUNKS)
    half = width // CORES
    dma = pltpu.SemaphoreType.DMA
    any_space = pl.BlockSpec(memory_space=pl.ANY)
    flops = 2 * rows * width * ff * 3
    return pl.pallas_call(
        functools.partial(reduce_kernel, n),
        name="reduce_terms",
        out_shape=[jax.ShapeDtypeStruct((rows, ff), BF16)] * 3 + [jax.ShapeDtypeStruct((rows, piece), BF16)],
        in_specs=[any_space] * 6,
        out_specs=[any_space] * 4,
        scratch_shapes=[
            pltpu.VMEM((width, 2 * ff), BF16),
            pltpu.VMEM((ff, width), BF16),
            pltpu.VMEM((rows, width), BF16),
            pltpu.VMEM((rows, 2 * ff), BF16),
            pltpu.VMEM((rows, ff), BF16),
            pltpu.VMEM((rows, half), BF16),
            pltpu.VMEM((rows, half), BF16),
            pltpu.VMEM((rows, piece), BF16),
            pltpu.VMEM((rows, piece), BF16),
            pltpu.VMEM((2, rows, piece), BF16),
            pltpu.VMEM((2, rows, piece), BF16),
            pltpu.VMEM((2, big // 2, piece), F32),
            pltpu.VMEM((2, big, piece), F32),
            pltpu.VMEM((rows, piece), BF16),
            dma((2, 4, 2)),
            dma((ff // piece,)),
            dma((steps, 3)),
            dma((steps, 3)),
            dma((steps,)),
            dma((steps, 4)),
            dma((steps, 4)),
            dma((steps, 2)),
            dma((steps, 2)),
            dma((steps, 2, 2)),
            dma((steps, 2, 2)),
        ],
        compiler_params=pltpu.CompilerParams(collective_id=0, has_side_effects=True, vmem_limit_bytes=60 * 2**20),
        cost_estimate=pl.CostEstimate(flops=flops, bytes_accessed=60 * 2**20, transcendentals=rows * ff),
    )(dy, gate, up, wg, wu, wd)


def weight_kernel(pairs, *refs):
    ins, outs = refs[: len(refs) - pairs], refs[len(refs) - pairs :]
    lhs = ins[0][...]
    for rhs, out in zip(ins[1:], outs):
        out[...] = lax.dot_general(lhs, rhs[...], CONTRACT_FIRST, preferred_element_type=F32).astype(BF16)


def weight_grads(name, lhs, rhss, bm, bn):
    k, m = lhs.shape
    nn = rhss[0].shape[1]
    count = len(rhss)
    return pl.pallas_call(
        functools.partial(weight_kernel, count),
        name=name,
        grid=(nn // bn, m // bm),
        out_shape=[jax.ShapeDtypeStruct((m, nn), BF16)] * count,
        in_specs=[pl.BlockSpec((k, bm), lambda j, i: (0, i))] + [pl.BlockSpec((k, bn), lambda j, i: (0, j))] * count,
        out_specs=[pl.BlockSpec((bm, bn), lambda j, i: (i, j))] * count,
        compiler_params=pltpu.CompilerParams(vmem_limit_bytes=40 * 2**20),
        cost_estimate=pl.CostEstimate(
            flops=2 * k * m * nn * count, bytes_accessed=2 * (k * m + (k + m) * nn * count), transcendentals=0
        ),
    )(lhs, *rhss)


def gather_kernel(n, *refs):
    pieces, out = refs[:-1], refs[-1]
    t = lax.axis_index("tp")
    chips = n // CORES
    chip, core = lax.div(t, CORES), lax.rem(t, CORES)
    width = pieces[0].shape[1]
    at = 0
    for other in range(CORES):
        for hop in (0, chips - 1, 1, 2):
            whose = lax.rem(core + other, CORES) * chips + lax.rem(chip + hop, chips)
            out[:, pl.ds(pl.multiple_of(whose * width, width), width)] = pieces[at][...]
            at += 1


def place(n, pieces, bm):
    rows, width = pieces[0].shape
    return pl.pallas_call(
        functools.partial(gather_kernel, n),
        name="place",
        grid=(rows // bm,),
        out_shape=jax.ShapeDtypeStruct((rows, width * n), BF16),
        in_specs=[pl.BlockSpec((bm, width), lambda i: (i, 0))] * n,
        out_specs=pl.BlockSpec((bm, width * n), lambda i: (i, 0)),
        cost_estimate=pl.CostEstimate(flops=0, bytes_accessed=4 * rows * width * n, transcendentals=0),
    )(*pieces)


def solution(mesh):
    n = mesh.shape["tp"]
    to_right = [(i, (i + CORES) % n) for i in range(n)]
    to_left = [(i, (i - CORES) % n) for i in range(n)]
    swap = [(i, i ^ 1) for i in range(n)]

    def send(v, where):
        return lax.ppermute(v, "tp", where)

    def step(x, dy, gate, up, w_gate, w_up, w_down):
        d_gate, d_up, hidden, red = reduce_terms(n, dy, gate, up, w_gate, w_up, w_down)
        h = red.shape[0] // 2
        top, bottom = red[:h], red[h:]
        from_left_top, from_right_bottom = send(top, to_right), send(bottom, to_left)
        from_left_bottom, from_right_top = send(bottom, to_right), send(top, to_left)
        other = send(red, swap)
        dw_gate, dw_up = weight_grads("dw_gate_up", x, [d_gate, d_up], 512, 1024)
        from_left_top, from_right_bottom, dw_gate, dw_up, hidden = lax.optimization_barrier(
            (from_left_top, from_right_bottom, dw_gate, dw_up, hidden)
        )
        far_top, far_bottom = send(from_left_top, to_right), send(from_right_bottom, to_left)
        (dw_down,) = weight_grads("dw_down", hidden, [dy], 512, 1024)
        far_top, far_bottom, from_left_bottom, from_right_top, other, dw_down = lax.optimization_barrier(
            (far_top, far_bottom, from_left_bottom, from_right_top, other, dw_down)
        )
        mine = [
            red,
            jnp.concatenate([from_left_top, from_left_bottom]),
            jnp.concatenate([from_right_top, from_right_bottom]),
            jnp.concatenate([far_top, far_bottom]),
        ]
        theirs = [other] + [send(v, swap) for v in mine[1:]]
        dx = place(n, mine + theirs, 512)
        return dx, dw_gate, dw_up, dw_down

    tokens, columns, rows = P("dp", None), P(None, "tp"), P("tp", None)
    return jax.shard_map(
        step,
        mesh=mesh,
        in_specs=(tokens, tokens, P("dp", "tp"), P("dp", "tp"), columns, columns, rows),
        out_specs=(tokens, P("dp", "tp"), P("dp", "tp"), P(("dp", "tp"), None)),
        check_vma=False,
    )
```

```python
import functools

import jax
import jax.numpy as jnp
from jax import lax
from jax.experimental import pallas as pl
from jax.experimental.pallas import tpu as pltpu
from jax.sharding import PartitionSpec as P


BF16, F32 = jnp.bfloat16, jnp.float32
CONTRACT_LAST = (((1,), (1,)), ((), ()))
CONTRACT_FIRST = (((0,), (0,)), ((), ()))
CORES = 2
GATE_UP_VMEM, DOWN_VMEM = 36 * 2**20, 40 * 2**20
CHUNKS = (256, 512, 512, 512, 256)
FAR, RIGHT, LEFT, OWN = range(4)
PAIRS = ((FAR, RIGHT), (LEFT, OWN))


def dot_tb(a, b):
    return lax.dot_general(a, b, CONTRACT_LAST, preferred_element_type=F32)


def product(a, b):
    return lax.dot_general(a, b, CONTRACT_FIRST, preferred_element_type=F32).astype(BF16)


def reduce_kernel(
    n, dy_hbm, gate_hbm, up_hbm, wg_hbm, wu_hbm, wd_hbm, d_hbm, hid_hbm, red_hbm, down_hbm,
    wcat, wd, dy, d, hid, psend, precv, fsend, frecv, nsend, nrecv, dep, own, red, down,
    wcat_sem, wd_sem, in_sem, out_sem, red_sem, down_sem, p_ssem, p_rsem, f_ssem, f_rsem, n_ssem, n_rsem,
):
    rows, width = dy.shape
    ff = wd.shape[0]
    piece = width // n
    chips = n // CORES
    steps = len(CHUNKS)

    t = lax.axis_index("tp")
    chip, core = lax.div(t, CORES), lax.rem(t, CORES)
    partner = t + 1 - 2 * core
    right, left = lax.rem(t + CORES, n), lax.rem(t + n - CORES, n)
    owner = [lax.rem(chip + hop, chips) for hop in (2, 1, chips - 1, 0)]

    def load_rows(i, r0, m):
        rr = pl.ds(r0, m)
        return [
            pltpu.make_async_copy(dy_hbm.at[rr], dy.at[rr], in_sem.at[i, 0]),
            pltpu.make_async_copy(gate_hbm.at[rr], d.at[rr, pl.ds(0, ff)], in_sem.at[i, 1]),
            pltpu.make_async_copy(up_hbm.at[rr], d.at[rr, pl.ds(ff, ff)], in_sem.at[i, 2]),
        ]

    blocks = ff // piece

    def load_wd(b):
        rr = pl.ds(b * piece, piece)
        return pltpu.make_async_copy(wd_hbm.at[rr], wd.at[rr], wd_sem.at[b])

    def load_wcat(half, j):
        whose = lax.rem(core + 1 + half, CORES)
        src = pl.ds(pl.multiple_of((whose * chips + owner[j]) * piece, piece), piece)
        dst = pl.ds((half * chips + j) * piece, piece)
        return [
            pltpu.make_async_copy(w.at[src], wcat.at[dst, pl.ds(k * ff, ff)], wcat_sem.at[half, j, k])
            for k, w in enumerate((wg_hbm, wu_hbm))
        ]

    def load_half(half):
        for j in range(4):
            for c in load_wcat(half, j):
                c.start()

    starts = [sum(CHUNKS[:i]) for i in range(steps)]
    for c in load_rows(0, starts[0], CHUNKS[0]):
        c.start()
    for b in range(blocks):
        load_wd(b).start()

    barrier = pltpu.get_barrier_semaphore()
    for other in (partner, left, right):
        pl.semaphore_signal(barrier, inc=1, device_id={"tp": other})

    def column(j):
        return pl.ds(j * piece, piece)

    def to_partner(i, r0, m, j):
        rr = pl.ds(r0, m)
        return pltpu.make_async_remote_copy(
            psend.at[rr, column(j)], precv.at[rr, column(j)], p_ssem.at[i, j], p_rsem.at[i, j], device_id={"tp": partner}
        )

    def far_copy(i, r0, m, side):
        rr = pl.ds(r0 + side * (m // 2), m // 2)
        return pltpu.make_async_remote_copy(
            fsend.at[rr], frecv.at[rr], f_ssem.at[i, side], f_rsem.at[i, side], device_id={"tp": (right, left)[side]}
        )

    def near_copy(i, r0, m, side, half):
        rr = pl.ds(r0 + half * (m // 2), m // 2)
        return pltpu.make_async_remote_copy(
            nsend.at[side, rr], nrecv.at[side, rr], n_ssem.at[i, side, half], n_rsem.at[i, side, half],
            device_id={"tp": (right, left)[side]},
        )

    def write_out(i, r0, m):
        rr = pl.ds(r0, m)
        return [
            pltpu.make_async_copy(d.at[rr], d_hbm.at[rr], out_sem.at[i, 0]),
            pltpu.make_async_copy(hid.at[rr], hid_hbm.at[rr], out_sem.at[i, 1]),
        ]

    def write_red(i, r0, m):
        rr = pl.ds(r0, m)
        return pltpu.make_async_copy(red.at[rr], red_hbm.at[rr], red_sem.at[i])

    def grads(i, r0, m, first=False, midway=None):
        rr = pl.ds(r0, m)
        with jax.named_scope("w_in"):
            for c in load_rows(i, r0, m):
                c.wait()
        if first:
            load_half(0)
            with jax.named_scope("w_wd"):
                for b in range(blocks):
                    load_wd(b).wait()
            load_half(1)
        for b in range(blocks):
            if midway and b == blocks // 2:
                midway()
            cg, cu = column(b), pl.ds(ff + b * piece, piece)
            dh = dot_tb(dy[rr, :], wd[column(b), :])
            g, u = d[rr, cg].astype(F32), d[rr, cu].astype(F32)
            s = jax.nn.sigmoid(g)
            silu = g * s
            hid[rr, cg] = (silu * u).astype(BF16)
            d[rr, cg] = (dh * u * (s + silu * (1.0 - s))).astype(BF16)
            d[rr, cu] = (dh * silu).astype(BF16)
        for c in write_out(i, r0, m):
            c.start()

    def exchange(i, r0, m, first=False):
        rr = pl.ds(r0, m)
        if first:
            for c in load_rows(1, starts[1], CHUNKS[1]):
                c.start()
            with jax.named_scope("w_bar"):
                pl.semaphore_wait(barrier, 3)
        for group in PAIRS:
            if first:
                with jax.named_scope("w_c0"):
                    for j in group:
                        for c in load_wcat(0, j):
                            c.wait()
            for j in group:
                psend[rr, column(j)] = dot_tb(d[rr, :], wcat[column(j), :]).astype(BF16)
            for j in group:
                to_partner(i, r0, m, j).start()

    def terms(i, r0, m, first=False):
        h = m // 2
        rr, top, bottom = pl.ds(r0, m), pl.ds(r0, h), pl.ds(r0 + h, h)
        for group in PAIRS:
            for j in group:
                if first:
                    with jax.named_scope("w_c1"):
                        for c in load_wcat(1, j):
                            c.wait()
                with jax.named_scope("w_p"):
                    to_partner(i, r0, m, j).wait_recv()
            for j in group:
                v = dot_tb(d[rr, :], wcat[column(chips + j), :]) + precv[rr, column(j)].astype(F32)
                if j == FAR:
                    fsend[rr, :] = v.astype(BF16)
                elif j == RIGHT:
                    nsend[0, bottom, :] = v[h:].astype(BF16)
                    dep[0, pl.ds(0, h), :] = v[:h]
                elif j == LEFT:
                    nsend[1, top, :] = v[:h].astype(BF16)
                    dep[1, pl.ds(0, h), :] = v[h:]
                else:
                    own[lax.rem(i, 2), pl.ds(0, m), :] = v
            if FAR in group:
                for side in range(2):
                    far_copy(i, r0, m, side).start()

    def direct(i, r0, m):
        near_copy(i, r0, m, 0, 1).start()
        near_copy(i, r0, m, 1, 0).start()

    def forward(i, r0, m):
        h = m // 2
        for side in range(2):
            rr = pl.ds(r0 + side * h, h)
            with jax.named_scope('w_f'):
                far_copy(i, r0, m, side).wait_recv()
            nsend[side, rr, :] = (dep[side, pl.ds(0, h), :] + frecv[rr, :].astype(F32)).astype(BF16)
            near_copy(i, r0, m, side, side).start()

    def finish(i, r0, m):
        rr = pl.ds(r0, m)
        for side in range(2):
            for half in range(2):
                with jax.named_scope('w_n'):
                    near_copy(i, r0, m, side, half).wait_recv()
        red[rr, :] = (own[lax.rem(i, 2), pl.ds(0, m), :] + nrecv[0, rr, :].astype(F32) + nrecv[1, rr, :].astype(F32)).astype(BF16)
        write_red(i, r0, m).start()

    half_ff = ff // 2

    def down_copy(q):
        rr = pl.ds(q * half_ff, half_ff)
        return pltpu.make_async_copy(down.at[rr], down_hbm.at[rr], down_sem.at[q])

    def down_part(q):
        down[pl.ds(q * half_ff, half_ff), :] = product(hid[:, pl.ds(q * half_ff, half_ff)], dy[:, pl.ds(0, down.shape[1])])
        down_copy(q).start()

    def step(i, r0, m, next_m, last_m, first=False):
        with jax.named_scope("terms"):
            terms(i, r0, m, first)
        if first:
            for k in range(2, steps):
                for c in load_rows(k, starts[k], CHUNKS[k]):
                    c.start()
        if next_m:
            with jax.named_scope("grads"):
                grads(i + 1, r0 + m, next_m, midway=lambda: direct(i, r0, m))
        else:
            with jax.named_scope("down"):
                down_part(0)
            with jax.named_scope("w_s"):
                for side in range(2):
                    far_copy(i, r0, m, side).wait_send()
            direct(i, r0, m)
        if next_m:
            with jax.named_scope("exchange"):
                exchange(i + 1, r0 + m, next_m)
        with jax.named_scope("forward"):
            forward(i, r0, m)
        if last_m:
            with jax.named_scope("finish"):
                finish(i - 1, r0 - last_m, last_m)

    with jax.named_scope("grads"):
        grads(0, 0, CHUNKS[0], True)
    with jax.named_scope("exchange"):
        exchange(0, 0, CHUNKS[0], True)
    i = 0
    while i < steps:
        key = (CHUNKS[i], CHUNKS[i + 1] if i + 1 < steps else 0, CHUNKS[i - 1] if i else 0)
        same = 1
        while 0 < i and i + same + 1 < steps and (CHUNKS[i + same], CHUNKS[i + same + 1], CHUNKS[i + same - 1]) == key:
            same += 1
        if same == 1:
            step(i, starts[i], *key, first=i == 0)
        else:
            base, r0, m = i, starts[i], CHUNKS[i]

            @pl.loop(0, same)
            def _(k):
                step(base + k, pl.multiple_of(r0 + k * m, piece), *key)

        i += same
    with jax.named_scope("down"):
        down_part(1)
    finish(steps - 1, starts[-1], CHUNKS[-1])
    for q in range(2):
        down_copy(q).wait()

    for i, (r0, m) in enumerate(zip(starts, CHUNKS)):
        for c in write_out(i, r0, m):
            c.wait()
        write_red(i, r0, m).wait()
        for j in range(4):
            to_partner(i, r0, m, j).wait_send()
        for side in range(2):
            if i + 1 < steps:
                far_copy(i, r0, m, side).wait_send()
            for half in range(2):
                near_copy(i, r0, m, side, half).wait_send()


def reduce_terms(n, dy, gate, up, wg, wu, wd):
    rows, width = dy.shape
    ff = gate.shape[1]
    piece = width // n
    steps = len(CHUNKS)
    big = max(CHUNKS)
    half = width // CORES
    dma = pltpu.SemaphoreType.DMA
    any_space = pl.BlockSpec(memory_space=pl.ANY)
    flops = 2 * rows * width * ff * 3
    return pl.pallas_call(
        functools.partial(reduce_kernel, n),
        name="reduce_terms",
        out_shape=[jax.ShapeDtypeStruct((rows, c), BF16) for c in (2 * ff, ff, piece)]
        + [jax.ShapeDtypeStruct((ff, half), BF16)],
        in_specs=[any_space] * 6,
        out_specs=[any_space] * 4,
        scratch_shapes=[
            pltpu.VMEM((width, 2 * ff), BF16),
            pltpu.VMEM((ff, width), BF16),
            pltpu.VMEM((rows, width), BF16),
            pltpu.VMEM((rows, 2 * ff), BF16),
            pltpu.VMEM((rows, ff), BF16),
            pltpu.VMEM((rows, half), BF16),
            pltpu.VMEM((rows, half), BF16),
            pltpu.VMEM((rows, piece), BF16),
            pltpu.VMEM((rows, piece), BF16),
            pltpu.VMEM((2, rows, piece), BF16),
            pltpu.VMEM((2, rows, piece), BF16),
            pltpu.VMEM((2, big // 2, piece), F32),
            pltpu.VMEM((2, big, piece), F32),
            pltpu.VMEM((rows, piece), BF16),
            pltpu.VMEM((ff, half), BF16),
            dma((2, 4, 2)),
            dma((ff // piece,)),
            dma((steps, 3)),
            dma((steps, 2)),
            dma((steps,)),
            dma((2,)),
            dma((steps, 4)),
            dma((steps, 4)),
            dma((steps, 2)),
            dma((steps, 2)),
            dma((steps, 2, 2)),
            dma((steps, 2, 2)),
        ],
        compiler_params=pltpu.CompilerParams(collective_id=0, has_side_effects=True, vmem_limit_bytes=60 * 2**20),
        cost_estimate=pl.CostEstimate(flops=flops, bytes_accessed=60 * 2**20, transcendentals=rows * ff),
    )(dy, gate, up, wg, wu, wd)


def gate_up_kernel(x, d, dw_gate, dw_up):
    @pl.when(pl.program_id(0) == 0)
    def _():
        dw_gate[...] = product(x[...], d[...])

    @pl.when(pl.program_id(0) == 1)
    def _():
        dw_up[...] = product(x[...], d[...])


def gate_up_grads(x, d, bm):
    k, m = x.shape
    ff = d.shape[1] // 2
    last = m // bm - 1
    return pl.pallas_call(
        gate_up_kernel,
        name="gate_up_grads",
        grid=(2, m // bm),
        out_shape=[jax.ShapeDtypeStruct((m, ff), BF16)] * 2,
        in_specs=[pl.BlockSpec((k, bm), lambda j, i: (0, i)), pl.BlockSpec((k, ff), lambda j, i: (0, j))],
        out_specs=[
            pl.BlockSpec((bm, ff), lambda j, i: (i * (1 - j) + last * j, 0)),
            pl.BlockSpec((bm, ff), lambda j, i: (i * j, 0)),
        ],
        compiler_params=pltpu.CompilerParams(vmem_limit_bytes=GATE_UP_VMEM),
        cost_estimate=pl.CostEstimate(flops=4 * k * m * ff, bytes_accessed=2 * (k * m + 2 * (k + m) * ff), transcendentals=0),
    )(x, d)


def own_columns(n, core_hop, chip_hop, width):
    t = lax.axis_index("tp")
    chips = n // CORES
    whose = lax.rem(lax.rem(t, CORES) + core_hop, CORES) * chips + lax.rem(lax.div(t, CORES) + chip_hop, chips)
    return pl.ds(pl.multiple_of(whose * width, width), width)


def piece_copies(n, hops, pieces, dx, held, in_sem, out_sem):
    reads = [pltpu.make_async_copy(p, held.at[q], in_sem.at[q]) for q, p in enumerate(pieces)]
    writes = [
        pltpu.make_async_copy(held.at[q], dx.at[:, own_columns(n, *hop, held.shape[2])], out_sem.at[q])
        for q, hop in enumerate(hops)
    ]
    return reads, writes


def down_kernel(n, hops, hidden_hbm, dy_hbm, part_hbm, *refs):
    count = len(hops)
    pieces = refs[:count]
    dw_down, dx, hidden, dy, out, part, held, load_sem, store_sem, part_sem, in_sem, out_sem = refs[count:]
    tiles, bm, width = out.shape
    ahead = part.shape[1]
    reads, writes = piece_copies(n, hops, pieces, dx, held, in_sem, out_sem)
    loads = [
        pltpu.make_async_copy(hidden_hbm.at[:, pl.ds(q * bm, bm)], hidden.at[q], load_sem.at[q]) for q in range(tiles)
    ]
    load_dy = pltpu.make_async_copy(dy_hbm.at[:, pl.ds(ahead, width)], dy, load_sem.at[tiles])
    load_part = pltpu.make_async_copy(part_hbm, part, part_sem.at[0])
    store_part = pltpu.make_async_copy(part, dw_down.at[:, pl.ds(0, ahead)], part_sem.at[1])
    stores = [
        pltpu.make_async_copy(out.at[q], dw_down.at[pl.ds(q * bm, bm), pl.ds(ahead, width)], store_sem.at[q])
        for q in range(tiles)
    ]
    loads[0].start()
    load_dy.start()
    loads[0].wait()
    load_dy.wait()
    for c in [*loads[1:], load_part, *reads]:
        c.start()
    for q in range(tiles):
        if q:
            loads[q].wait()
        out[q] = product(hidden[q], dy[...])
        stores[q].start()
        if q == 0:
            load_part.wait()
            store_part.start()
            for r, w in zip(reads, writes):
                r.wait()
                w.start()
    for c in [store_part, *stores, *writes]:
        c.wait()


def down_grad(n, hidden, dy, part, hops, pieces, bm):
    k, ff = hidden.shape
    width, ahead = dy.shape[1], part.shape[1]
    rows, piece = pieces[0].shape
    any_space = pl.BlockSpec(memory_space=pl.ANY)
    dma = pltpu.SemaphoreType.DMA
    tiles, rest = ff // bm, width - ahead
    return pl.pallas_call(
        functools.partial(down_kernel, n, hops),
        name="down_grad",
        out_shape=[jax.ShapeDtypeStruct((ff, width), BF16), jax.ShapeDtypeStruct((rows, piece * n), BF16)],
        in_specs=[pl.BlockSpec(memory_space=pltpu.HBM)] * 3 + [any_space] * len(pieces),
        out_specs=[any_space] * 2,
        scratch_shapes=[
            pltpu.VMEM((tiles, k, bm), BF16),
            pltpu.VMEM((k, rest), BF16),
            pltpu.VMEM((tiles, bm, rest), BF16),
            pltpu.VMEM((ff, ahead), BF16),
            pltpu.VMEM((len(pieces), rows, piece), BF16),
            dma((tiles + 1,)),
            dma((tiles,)),
            dma((2,)),
            dma((len(pieces),)),
            dma((len(pieces),)),
        ],
        compiler_params=pltpu.CompilerParams(vmem_limit_bytes=DOWN_VMEM),
        cost_estimate=pl.CostEstimate(flops=2 * k * ff * rest, bytes_accessed=2 * (k * ff + (k + ff) * width), transcendentals=0),
    )(hidden, dy, part, *pieces)


def place_kernel(n, hops, *refs):
    count = len(hops)
    pieces, (dx, sem) = refs[:count], refs[count + 1 :]
    writes = [
        pltpu.make_async_copy(p, dx.at[pl.ds(row, p.shape[0]), own_columns(n, *hop, p.shape[1])], sem.at[q])
        for q, (p, (row, *hop)) in enumerate(zip(pieces, hops))
    ]
    for c in writes:
        c.start()
    for c in writes:
        c.wait()


def place(n, hops, pieces, dx):
    any_space = pl.BlockSpec(memory_space=pl.ANY)
    return pl.pallas_call(
        functools.partial(place_kernel, n, hops),
        name="place",
        out_shape=jax.ShapeDtypeStruct(dx.shape, BF16),
        in_specs=[pl.BlockSpec(memory_space=pltpu.VMEM)] * len(pieces) + [any_space],
        out_specs=any_space,
        input_output_aliases={len(pieces): 0},
        scratch_shapes=[pltpu.SemaphoreType.DMA((len(pieces),))],
        compiler_params=pltpu.CompilerParams(vmem_limit_bytes=16 * 2**20),
        cost_estimate=pl.CostEstimate(flops=0, bytes_accessed=sum(4 * p.size for p in pieces), transcendentals=0),
    )(*pieces, dx)


def solution(mesh):
    n = mesh.shape["tp"]
    to_right = [(i, (i + CORES) % n) for i in range(n)]
    to_left = [(i, (i - CORES) % n) for i in range(n)]
    swap = [(i, i ^ 1) for i in range(n)]

    def send(v, where):
        return lax.ppermute(v, "tp", where)

    def step(x, dy, gate, up, w_gate, w_up, w_down):
        d, hidden, red, part = reduce_terms(n, dy, gate, up, w_gate, w_up, w_down)
        h = red.shape[0] // 2
        chips = n // CORES
        from_left, from_right, other = send(red, to_right), send(red, to_left), send(red, swap)
        dw_gate, dw_up = gate_up_grads(*(pltpu.with_memory_space_constraint(v, pltpu.HBM) for v in (x, d)), 512)
        from_left, from_right, other, dw_gate, dw_up, hidden = lax.optimization_barrier(
            (from_left, from_right, other, dw_gate, dw_up, hidden)
        )
        far = send(from_left[:h], to_right), send(from_right[h:], to_left)
        left2, right2 = send(from_left, swap), send(from_right, swap)
        dw_down, dx = down_grad(
            n, hidden, dy, part, ((0, 0), (1, 0), (0, chips - 1), (0, 1)), (red, other, from_left, from_right), 512
        )
        far, left2, right2, dw_down, dx = lax.optimization_barrier((far, left2, right2, dw_down, dx))
        far2 = [send(v, swap) for v in far]
        hops = ((0, 1, chips - 1), (0, 1, 1), (0, 0, 2), (h, 0, 2), (0, 1, 2), (h, 1, 2))
        dx = place(n, hops, (left2, right2, *far, *far2), dx)
        return dx, dw_gate, dw_up, dw_down

    tokens, columns, rows = P("dp", None), P(None, "tp"), P("tp", None)
    return jax.shard_map(
        step,
        mesh=mesh,
        in_specs=(tokens, tokens, P("dp", "tp"), P("dp", "tp"), columns, columns, rows),
        out_specs=(tokens, P("dp", "tp"), P("dp", "tp"), P(("dp", "tp"), None)),
        check_vma=False,
    )
```

```python
import functools

import jax
import jax.numpy as jnp
from jax import lax
from jax.experimental import pallas as pl
from jax.experimental.pallas import tpu as pltpu
from jax.sharding import PartitionSpec as P


BF16, F32 = jnp.bfloat16, jnp.float32
CONTRACT_LAST = (((1,), (1,)), ((), ()))
CONTRACT_FIRST = (((0,), (0,)), ((), ()))
CORES = 2
GATE_UP_VMEM, DOWN_VMEM = 36 * 2**20, 40 * 2**20
CHUNKS = (256, 384, 384, 384, 384, 256)
FAR, RIGHT, LEFT, OWN = range(4)
PAIRS = ((FAR, RIGHT), (LEFT, OWN))


def dot_tb(a, b):
    return lax.dot_general(a, b, CONTRACT_LAST, preferred_element_type=F32)


def product(a, b):
    return lax.dot_general(a, b, CONTRACT_FIRST, preferred_element_type=F32).astype(BF16)


def reduce_kernel(
    n, dy_hbm, gate_hbm, up_hbm, wg_hbm, wu_hbm, wd_hbm, d_hbm, hid_hbm, red_hbm, down_hbm,
    wcat, wd, dy, d, hid, psend, precv, fsend, frecv, nsend, nrecv, dep, own, red, down,
    wcat_sem, wd_sem, in_sem, out_sem, red_sem, down_sem, p_ssem, p_rsem, f_ssem, f_rsem, n_ssem, n_rsem,
):
    rows, width = dy.shape
    ff = wd.shape[0]
    piece = width // n
    chips = n // CORES
    steps = len(CHUNKS)

    t = lax.axis_index("tp")
    chip, core = lax.div(t, CORES), lax.rem(t, CORES)
    partner = t + 1 - 2 * core
    right, left = lax.rem(t + CORES, n), lax.rem(t + n - CORES, n)
    owner = [lax.rem(chip + hop, chips) for hop in (2, 1, chips - 1, 0)]

    def load_rows(i, r0, m):
        rr = pl.ds(r0, m)
        return [
            pltpu.make_async_copy(dy_hbm.at[rr], dy.at[rr], in_sem.at[i, 0]),
            pltpu.make_async_copy(gate_hbm.at[rr], d.at[rr, pl.ds(0, ff)], in_sem.at[i, 1]),
            pltpu.make_async_copy(up_hbm.at[rr], d.at[rr, pl.ds(ff, ff)], in_sem.at[i, 2]),
        ]

    blocks = ff // piece

    def load_wd(b):
        rr = pl.ds(b * piece, piece)
        return pltpu.make_async_copy(wd_hbm.at[rr], wd.at[rr], wd_sem.at[b])

    def load_wcat(half, j):
        whose = lax.rem(core + 1 + half, CORES)
        src = pl.ds(pl.multiple_of((whose * chips + owner[j]) * piece, piece), piece)
        dst = pl.ds((half * chips + j) * piece, piece)
        return [
            pltpu.make_async_copy(w.at[src], wcat.at[dst, pl.ds(k * ff, ff)], wcat_sem.at[half, j, k])
            for k, w in enumerate((wg_hbm, wu_hbm))
        ]

    def load_half(half):
        for j in range(4):
            for c in load_wcat(half, j):
                c.start()

    starts = [sum(CHUNKS[:i]) for i in range(steps)]
    for c in load_rows(0, starts[0], CHUNKS[0]):
        c.start()
    for b in range(blocks):
        load_wd(b).start()

    barrier = pltpu.get_barrier_semaphore()
    for other in (partner, left, right):
        pl.semaphore_signal(barrier, inc=1, device_id={"tp": other})

    def column(j):
        return pl.ds(j * piece, piece)

    def to_partner(i, r0, m, j):
        rr = pl.ds(r0, m)
        return pltpu.make_async_remote_copy(
            psend.at[rr, column(j)], precv.at[rr, column(j)], p_ssem.at[i, j], p_rsem.at[i, j], device_id={"tp": partner}
        )

    def far_copy(i, r0, m, side):
        rr = pl.ds(r0 + side * (m // 2), m // 2)
        return pltpu.make_async_remote_copy(
            fsend.at[rr], frecv.at[rr], f_ssem.at[i, side], f_rsem.at[i, side], device_id={"tp": (right, left)[side]}
        )

    def near_copy(i, r0, m, side, half):
        rr = pl.ds(r0 + half * (m // 2), m // 2)
        return pltpu.make_async_remote_copy(
            nsend.at[side, rr], nrecv.at[side, rr], n_ssem.at[i, side, half], n_rsem.at[i, side, half],
            device_id={"tp": (right, left)[side]},
        )

    def write_out(i, r0, m):
        rr = pl.ds(r0, m)
        return [
            pltpu.make_async_copy(d.at[rr], d_hbm.at[rr], out_sem.at[i, 0]),
            pltpu.make_async_copy(hid.at[rr], hid_hbm.at[rr], out_sem.at[i, 1]),
        ]

    def write_red(i, r0, m):
        rr = pl.ds(r0, m)
        return pltpu.make_async_copy(red.at[rr], red_hbm.at[rr], red_sem.at[i])

    def grads(i, r0, m, first=False, midway=None):
        rr = pl.ds(r0, m)
        with jax.named_scope("w_in"):
            for c in load_rows(i, r0, m):
                c.wait()
        if first:
            load_half(0)
            with jax.named_scope("w_wd"):
                for b in range(blocks):
                    load_wd(b).wait()
            load_half(1)
        for b in range(blocks):
            if midway and b == blocks // 2:
                midway()
            cg, cu = column(b), pl.ds(ff + b * piece, piece)
            dh = dot_tb(dy[rr, :], wd[column(b), :])
            g, u = d[rr, cg].astype(F32), d[rr, cu].astype(F32)
            s = jax.nn.sigmoid(g)
            silu = g * s
            hid[rr, cg] = (silu * u).astype(BF16)
            d[rr, cg] = (dh * u * (s + silu * (1.0 - s))).astype(BF16)
            d[rr, cu] = (dh * silu).astype(BF16)
        for c in write_out(i, r0, m):
            c.start()

    def exchange(i, r0, m, first=False):
        rr = pl.ds(r0, m)
        if first:
            for c in load_rows(1, starts[1], CHUNKS[1]):
                c.start()
            with jax.named_scope("w_bar"):
                pl.semaphore_wait(barrier, 3)
        for group in PAIRS:
            if first:
                with jax.named_scope("w_c0"):
                    for j in group:
                        for c in load_wcat(0, j):
                            c.wait()
            for j in group:
                psend[rr, column(j)] = dot_tb(d[rr, :], wcat[column(j), :]).astype(BF16)
            for j in group:
                to_partner(i, r0, m, j).start()

    def terms(i, r0, m, first=False):
        h = m // 2
        rr, top, bottom = pl.ds(r0, m), pl.ds(r0, h), pl.ds(r0 + h, h)
        for group in PAIRS:
            for j in group:
                if first:
                    with jax.named_scope("w_c1"):
                        for c in load_wcat(1, j):
                            c.wait()
                with jax.named_scope("w_p"):
                    to_partner(i, r0, m, j).wait_recv()
            for j in group:
                v = dot_tb(d[rr, :], wcat[column(chips + j), :]) + precv[rr, column(j)].astype(F32)
                if j == FAR:
                    fsend[rr, :] = v.astype(BF16)
                elif j == RIGHT:
                    nsend[0, bottom, :] = v[h:].astype(BF16)
                    dep[0, pl.ds(0, h), :] = v[:h]
                elif j == LEFT:
                    nsend[1, top, :] = v[:h].astype(BF16)
                    dep[1, pl.ds(0, h), :] = v[h:]
                else:
                    own[lax.rem(i, 2), pl.ds(0, m), :] = v
            if FAR in group:
                for side in range(2):
                    far_copy(i, r0, m, side).start()

    def direct(i, r0, m):
        near_copy(i, r0, m, 0, 1).start()
        near_copy(i, r0, m, 1, 0).start()

    def forward(i, r0, m):
        h = m // 2
        for side in range(2):
            rr = pl.ds(r0 + side * h, h)
            with jax.named_scope('w_f'):
                far_copy(i, r0, m, side).wait_recv()
            nsend[side, rr, :] = (dep[side, pl.ds(0, h), :] + frecv[rr, :].astype(F32)).astype(BF16)
            near_copy(i, r0, m, side, side).start()

    def finish(i, r0, m):
        rr = pl.ds(r0, m)
        for side in range(2):
            for half in range(2):
                with jax.named_scope('w_n'):
                    near_copy(i, r0, m, side, half).wait_recv()
        red[rr, :] = (own[lax.rem(i, 2), pl.ds(0, m), :] + nrecv[0, rr, :].astype(F32) + nrecv[1, rr, :].astype(F32)).astype(BF16)
        write_red(i, r0, m).start()

    half_ff = ff // 2

    def down_copy(q):
        rr = pl.ds(pl.multiple_of(q * half_ff, half_ff), half_ff)
        return pltpu.make_async_copy(down.at[rr], down_hbm.at[rr], down_sem.at[q])

    def down_part(q):
        part = pl.ds(pl.multiple_of(q * half_ff, half_ff), half_ff)
        down[part, :] = product(hid[:, part], dy[:, pl.ds(0, down.shape[1])])
        down_copy(q).start()

    def step(i, r0, m, next_m, last_m, first=False):
        with jax.named_scope("terms"):
            terms(i, r0, m, first)
        if first:
            for k in range(2, steps):
                for c in load_rows(k, starts[k], CHUNKS[k]):
                    c.start()
        if next_m:
            with jax.named_scope("grads"):
                grads(i + 1, r0 + m, next_m, midway=lambda: direct(i, r0, m))
            with jax.named_scope("exchange"):
                exchange(i + 1, r0 + m, next_m)
            settle(i, r0, m, last_m)
            return

        @pl.loop(0, 2)
        def _(q):
            with jax.named_scope("down"):
                down_part(q)

            @pl.when(q == 0)
            def _():
                for side in range(2):
                    far_copy(i, r0, m, side).wait_send()
                direct(i, r0, m)
                settle(i, r0, m, last_m)

    def settle(i, r0, m, last_m):
        with jax.named_scope("forward"):
            forward(i, r0, m)
        if last_m:
            with jax.named_scope("finish"):
                finish(i - 1, r0 - last_m, last_m)

    with jax.named_scope("grads"):
        grads(0, 0, CHUNKS[0], True)
    with jax.named_scope("exchange"):
        exchange(0, 0, CHUNKS[0], True)
    i = 0
    while i < steps:
        key = (CHUNKS[i], CHUNKS[i + 1] if i + 1 < steps else 0, CHUNKS[i - 1] if i else 0)
        same = 1
        while 0 < i and i + same + 1 < steps and (CHUNKS[i + same], CHUNKS[i + same + 1], CHUNKS[i + same - 1]) == key:
            same += 1
        if same == 1:
            step(i, starts[i], *key, first=i == 0)
        else:
            base, r0, m = i, starts[i], CHUNKS[i]

            @pl.loop(0, same)
            def _(k):
                step(base + k, pl.multiple_of(r0 + k * m, 128), *key)

        i += same
    finish(steps - 1, starts[-1], CHUNKS[-1])
    for q in range(2):
        down_copy(q).wait()

    for i, (r0, m) in enumerate(zip(starts, CHUNKS)):
        for c in write_out(i, r0, m):
            c.wait()
        write_red(i, r0, m).wait()
        for j in range(4):
            to_partner(i, r0, m, j).wait_send()
        for side in range(2):
            if i + 1 < steps:
                far_copy(i, r0, m, side).wait_send()
            for half in range(2):
                near_copy(i, r0, m, side, half).wait_send()


def reduce_terms(n, dy, gate, up, wg, wu, wd):
    rows, width = dy.shape
    ff = gate.shape[1]
    piece = width // n
    steps = len(CHUNKS)
    big = max(CHUNKS)
    half = width // CORES
    dma = pltpu.SemaphoreType.DMA
    any_space = pl.BlockSpec(memory_space=pl.ANY)
    flops = 2 * rows * width * ff * 3
    return pl.pallas_call(
        functools.partial(reduce_kernel, n),
        name="reduce_terms",
        out_shape=[jax.ShapeDtypeStruct((rows, c), BF16) for c in (2 * ff, ff, piece)]
        + [jax.ShapeDtypeStruct((ff, half), BF16)],
        in_specs=[any_space] * 6,
        out_specs=[any_space] * 4,
        scratch_shapes=[
            pltpu.VMEM((width, 2 * ff), BF16),
            pltpu.VMEM((ff, width), BF16),
            pltpu.VMEM((rows, width), BF16),
            pltpu.VMEM((rows, 2 * ff), BF16),
            pltpu.VMEM((rows, ff), BF16),
            pltpu.VMEM((rows, half), BF16),
            pltpu.VMEM((rows, half), BF16),
            pltpu.VMEM((rows, piece), BF16),
            pltpu.VMEM((rows, piece), BF16),
            pltpu.VMEM((2, rows, piece), BF16),
            pltpu.VMEM((2, rows, piece), BF16),
            pltpu.VMEM((2, big // 2, piece), F32),
            pltpu.VMEM((2, big, piece), F32),
            pltpu.VMEM((rows, piece), BF16),
            pltpu.VMEM((ff, half), BF16),
            dma((2, 4, 2)),
            dma((ff // piece,)),
            dma((steps, 3)),
            dma((steps, 2)),
            dma((steps,)),
            dma((2,)),
            dma((steps, 4)),
            dma((steps, 4)),
            dma((steps, 2)),
            dma((steps, 2)),
            dma((steps, 2, 2)),
            dma((steps, 2, 2)),
        ],
        compiler_params=pltpu.CompilerParams(collective_id=0, has_side_effects=True, vmem_limit_bytes=60 * 2**20),
        cost_estimate=pl.CostEstimate(flops=flops, bytes_accessed=60 * 2**20, transcendentals=rows * ff),
    )(dy, gate, up, wg, wu, wd)


def gate_up_kernel(x, d, dw_gate, dw_up):
    @pl.when(pl.program_id(0) == 0)
    def _():
        dw_gate[...] = product(x[...], d[...])

    @pl.when(pl.program_id(0) == 1)
    def _():
        dw_up[...] = product(x[...], d[...])


def gate_up_grads(x, d, bm):
    k, m = x.shape
    ff = d.shape[1] // 2
    last = m // bm - 1
    return pl.pallas_call(
        gate_up_kernel,
        name="gate_up_grads",
        grid=(2, m // bm),
        out_shape=[jax.ShapeDtypeStruct((m, ff), BF16)] * 2,
        in_specs=[pl.BlockSpec((k, bm), lambda j, i: (0, i)), pl.BlockSpec((k, ff), lambda j, i: (0, j))],
        out_specs=[
            pl.BlockSpec((bm, ff), lambda j, i: (i * (1 - j) + last * j, 0)),
            pl.BlockSpec((bm, ff), lambda j, i: (i * j, 0)),
        ],
        compiler_params=pltpu.CompilerParams(vmem_limit_bytes=GATE_UP_VMEM),
        cost_estimate=pl.CostEstimate(flops=4 * k * m * ff, bytes_accessed=2 * (k * m + 2 * (k + m) * ff), transcendentals=0),
    )(x, d)


def own_columns(n, core_hop, chip_hop, width):
    t = lax.axis_index("tp")
    chips = n // CORES
    whose = lax.rem(lax.rem(t, CORES) + core_hop, CORES) * chips + lax.rem(lax.div(t, CORES) + chip_hop, chips)
    return pl.ds(pl.multiple_of(whose * width, width), width)


def piece_copies(n, hops, pieces, dx, held, in_sem, out_sem):
    reads = [pltpu.make_async_copy(p, held.at[q], in_sem.at[q]) for q, p in enumerate(pieces)]
    writes = [
        pltpu.make_async_copy(held.at[q], dx.at[:, own_columns(n, *hop, held.shape[2])], out_sem.at[q])
        for q, hop in enumerate(hops)
    ]
    return reads, writes


def down_kernel(n, hops, hidden_hbm, dy_hbm, part_hbm, *refs):
    count = len(hops)
    pieces = refs[:count]
    dw_down, dx, hidden, dy, out, part, held, load_sem, store_sem, part_sem, in_sem, out_sem = refs[count:]
    tiles, bm, width = out.shape
    ahead = part.shape[1]
    reads, writes = piece_copies(n, hops, pieces, dx, held, in_sem, out_sem)
    def load(q):
        return pltpu.make_async_copy(hidden_hbm.at[:, pl.ds(pl.multiple_of(q * bm, bm), bm)], hidden.at[q], load_sem.at[q])

    def store(q):
        rr = pl.ds(pl.multiple_of(q * bm, bm), bm)
        return pltpu.make_async_copy(out.at[q], dw_down.at[rr, pl.ds(ahead, width)], store_sem.at[q])

    load_dy = pltpu.make_async_copy(dy_hbm.at[:, pl.ds(ahead, width)], dy, load_sem.at[tiles])
    load_part = pltpu.make_async_copy(part_hbm, part, part_sem.at[0])
    store_part = pltpu.make_async_copy(part, dw_down.at[:, pl.ds(0, ahead)], part_sem.at[1])
    load(0).start()
    load_dy.start()
    load(0).wait()
    load_dy.wait()
    for c in [*(load(q) for q in range(1, tiles)), load_part, *reads]:
        c.start()

    @pl.loop(0, tiles)
    def _(q):
        @pl.when(q > 0)
        def _():
            load(q).wait()

        out[q] = product(hidden[q], dy[...])
        store(q).start()

        @pl.when(q == 0)
        def _():
            load_part.wait()
            store_part.start()
            for r, w in zip(reads, writes):
                r.wait()
                w.start()

    for c in [store_part, *(store(q) for q in range(tiles)), *writes]:
        c.wait()


def down_grad(n, hidden, dy, part, hops, pieces, bm):
    k, ff = hidden.shape
    width, ahead = dy.shape[1], part.shape[1]
    rows, piece = pieces[0].shape
    any_space = pl.BlockSpec(memory_space=pl.ANY)
    dma = pltpu.SemaphoreType.DMA
    tiles, rest = ff // bm, width - ahead
    return pl.pallas_call(
        functools.partial(down_kernel, n, hops),
        name="down_grad",
        out_shape=[jax.ShapeDtypeStruct((ff, width), BF16), jax.ShapeDtypeStruct((rows, piece * n), BF16)],
        in_specs=[pl.BlockSpec(memory_space=pltpu.HBM)] * 3 + [any_space] * len(pieces),
        out_specs=[any_space] * 2,
        scratch_shapes=[
            pltpu.VMEM((tiles, k, bm), BF16),
            pltpu.VMEM((k, rest), BF16),
            pltpu.VMEM((tiles, bm, rest), BF16),
            pltpu.VMEM((ff, ahead), BF16),
            pltpu.VMEM((len(pieces), rows, piece), BF16),
            dma((tiles + 1,)),
            dma((tiles,)),
            dma((2,)),
            dma((len(pieces),)),
            dma((len(pieces),)),
        ],
        compiler_params=pltpu.CompilerParams(vmem_limit_bytes=DOWN_VMEM),
        cost_estimate=pl.CostEstimate(flops=2 * k * ff * rest, bytes_accessed=2 * (k * ff + (k + ff) * width), transcendentals=0),
    )(hidden, dy, part, *pieces)


def place_kernel(n, hops, *refs):
    count = len(hops)
    pieces, (dx, sem) = refs[:count], refs[count + 1 :]
    writes = [
        pltpu.make_async_copy(p, dx.at[pl.ds(row, p.shape[0]), own_columns(n, *hop, p.shape[1])], sem.at[q])
        for q, (p, (row, *hop)) in enumerate(zip(pieces, hops))
    ]
    for c in writes:
        c.start()
    for c in writes:
        c.wait()


def place(n, hops, pieces, dx):
    any_space = pl.BlockSpec(memory_space=pl.ANY)
    return pl.pallas_call(
        functools.partial(place_kernel, n, hops),
        name="place",
        out_shape=jax.ShapeDtypeStruct(dx.shape, BF16),
        in_specs=[pl.BlockSpec(memory_space=pltpu.VMEM)] * len(pieces) + [any_space],
        out_specs=any_space,
        input_output_aliases={len(pieces): 0},
        scratch_shapes=[pltpu.SemaphoreType.DMA((len(pieces),))],
        compiler_params=pltpu.CompilerParams(vmem_limit_bytes=16 * 2**20),
        cost_estimate=pl.CostEstimate(flops=0, bytes_accessed=sum(4 * p.size for p in pieces), transcendentals=0),
    )(*pieces, dx)


def solution(mesh):
    n = mesh.shape["tp"]
    to_right = [(i, (i + CORES) % n) for i in range(n)]
    to_left = [(i, (i - CORES) % n) for i in range(n)]
    swap = [(i, i ^ 1) for i in range(n)]

    def send(v, where):
        return lax.ppermute(v, "tp", where)

    def step(x, dy, gate, up, w_gate, w_up, w_down):
        d, hidden, red, part = reduce_terms(n, dy, gate, up, w_gate, w_up, w_down)
        h = red.shape[0] // 2
        chips = n // CORES
        from_left, from_right, other = send(red, to_right), send(red, to_left), send(red, swap)
        dw_gate, dw_up = gate_up_grads(*(pltpu.with_memory_space_constraint(v, pltpu.HBM) for v in (x, d)), 512)
        from_left, from_right, other, dw_gate, dw_up, hidden = lax.optimization_barrier(
            (from_left, from_right, other, dw_gate, dw_up, hidden)
        )
        far = send(from_left[:h], to_right), send(from_right[h:], to_left)
        left2, right2 = send(from_left, swap), send(from_right, swap)
        dw_down, dx = down_grad(
            n, hidden, dy, part, ((0, 0), (1, 0), (0, chips - 1), (0, 1)), (red, other, from_left, from_right), 512
        )
        far, left2, right2, dw_down, dx = lax.optimization_barrier((far, left2, right2, dw_down, dx))
        far2 = [send(v, swap) for v in far]
        hops = ((0, 1, chips - 1), (0, 1, 1), (0, 0, 2), (h, 0, 2), (0, 1, 2), (h, 1, 2))
        dx = place(n, hops, (left2, right2, *far, *far2), dx)
        return dx, dw_gate, dw_up, dw_down

    tokens, columns, rows = P("dp", None), P(None, "tp"), P("tp", None)
    return jax.shard_map(
        step,
        mesh=mesh,
        in_specs=(tokens, tokens, P("dp", "tp"), P("dp", "tp"), columns, columns, rows),
        out_specs=(tokens, P("dp", "tp"), P("dp", "tp"), P(("dp", "tp"), None)),
        check_vma=False,
    )
```

```python
import functools

import jax
import jax.numpy as jnp
from jax import lax
from jax.experimental import pallas as pl
from jax.experimental.pallas import tpu as pltpu
from jax.sharding import PartitionSpec as P


BF16, F32 = jnp.bfloat16, jnp.float32
CONTRACT_LAST = (((1,), (1,)), ((), ()))
CONTRACT_FIRST = (((0,), (0,)), ((), ()))
CORES = 2
GATE_UP_VMEM, DOWN_VMEM = 36 * 2**20, 40 * 2**20
CHUNKS = (256, 384, 384, 384, 384, 256)
FAR, RIGHT, LEFT, OWN = range(4)
PAIRS = ((FAR, RIGHT), (LEFT, OWN))


def dot_tb(a, b):
    return lax.dot_general(a, b, CONTRACT_LAST, preferred_element_type=F32)


def product(a, b):
    return lax.dot_general(a, b, CONTRACT_FIRST, preferred_element_type=F32).astype(BF16)


def reduce_kernel(
    n, dy_hbm, gate_hbm, up_hbm, wg_hbm, wu_hbm, wd_hbm, d_hbm, hid_hbm, red_hbm, down_hbm,
    wcat, wd, dy, d, hid, psend, precv, fsend, frecv, nsend, nrecv, dep, own, red, down,
    wcat_sem, wd_sem, in_sem, out_sem, red_sem, down_sem, p_ssem, p_rsem, f_ssem, f_rsem, n_ssem, n_rsem,
):
    rows, width = dy.shape
    ff = wd.shape[0]
    piece = width // n
    chips = n // CORES
    steps = len(CHUNKS)

    t = lax.axis_index("tp")
    chip, core = lax.div(t, CORES), lax.rem(t, CORES)
    partner = t + 1 - 2 * core
    right, left = lax.rem(t + CORES, n), lax.rem(t + n - CORES, n)
    owner = [lax.rem(chip + hop, chips) for hop in (2, 1, chips - 1, 0)]

    def load_rows(i, r0, m):
        rr = pl.ds(r0, m)
        return [
            pltpu.make_async_copy(dy_hbm.at[rr], dy.at[rr], in_sem.at[i, 0]),
            pltpu.make_async_copy(gate_hbm.at[rr], d.at[rr, pl.ds(0, ff)], in_sem.at[i, 1]),
            pltpu.make_async_copy(up_hbm.at[rr], d.at[rr, pl.ds(ff, ff)], in_sem.at[i, 2]),
        ]

    blocks = ff // piece

    def load_wd(b):
        rr = pl.ds(b * piece, piece)
        return pltpu.make_async_copy(wd_hbm.at[rr], wd.at[rr], wd_sem.at[b])

    def load_wcat(half, j):
        whose = lax.rem(core + 1 + half, CORES)
        src = pl.ds(pl.multiple_of((whose * chips + owner[j]) * piece, piece), piece)
        dst = pl.ds((half * chips + j) * piece, piece)
        return [
            pltpu.make_async_copy(w.at[src], wcat.at[dst, pl.ds(k * ff, ff)], wcat_sem.at[half, j, k])
            for k, w in enumerate((wg_hbm, wu_hbm))
        ]

    def load_half(half):
        for j in range(4):
            for c in load_wcat(half, j):
                c.start()

    starts = [sum(CHUNKS[:i]) for i in range(steps)]
    for c in load_rows(0, starts[0], CHUNKS[0]):
        c.start()
    for b in range(blocks):
        load_wd(b).start()

    barrier = pltpu.get_barrier_semaphore()
    for other in (partner, left, right):
        pl.semaphore_signal(barrier, inc=1, device_id={"tp": other})

    def column(j):
        return pl.ds(j * piece, piece)

    def to_partner(i, r0, m, j):
        rr = pl.ds(r0, m)
        return pltpu.make_async_remote_copy(
            psend.at[rr, column(j)], precv.at[rr, column(j)], p_ssem.at[i, j], p_rsem.at[i, j], device_id={"tp": partner}
        )

    def far_copy(i, r0, m, side):
        rr = pl.ds(r0 + side * (m // 2), m // 2)
        return pltpu.make_async_remote_copy(
            fsend.at[rr], frecv.at[rr], f_ssem.at[i, side], f_rsem.at[i, side], device_id={"tp": (right, left)[side]}
        )

    def near_copy(i, r0, m, side, half):
        rr = pl.ds(r0 + half * (m // 2), m // 2)
        return pltpu.make_async_remote_copy(
            nsend.at[side, rr], nrecv.at[side, rr], n_ssem.at[i, side, half], n_rsem.at[i, side, half],
            device_id={"tp": (right, left)[side]},
        )

    def write_out(i, r0, m):
        rr = pl.ds(r0, m)
        return [
            pltpu.make_async_copy(d.at[rr], d_hbm.at[rr], out_sem.at[i, 0]),
            pltpu.make_async_copy(hid.at[rr], hid_hbm.at[rr], out_sem.at[i, 1]),
        ]

    def write_red(i, r0, m):
        rr = pl.ds(r0, m)
        return pltpu.make_async_copy(red.at[rr], red_hbm.at[rr], red_sem.at[i])

    def grads(i, r0, m, first=False):
        rr = pl.ds(r0, m)
        with jax.named_scope("w_in"):
            for c in load_rows(i, r0, m):
                c.wait()
        if first:
            load_half(0)
            with jax.named_scope("w_wd"):
                for b in range(blocks):
                    load_wd(b).wait()
            load_half(1)
        for b in range(blocks):
            cg, cu = column(b), pl.ds(ff + b * piece, piece)
            dh = dot_tb(dy[rr, :], wd[column(b), :])
            g, u = d[rr, cg].astype(F32), d[rr, cu].astype(F32)
            s = jax.nn.sigmoid(g)
            silu = g * s
            hid[rr, cg] = (silu * u).astype(BF16)
            d[rr, cg] = (dh * u * (s + silu * (1.0 - s))).astype(BF16)
            d[rr, cu] = (dh * silu).astype(BF16)
        for c in write_out(i, r0, m):
            c.start()

    def exchange(i, r0, m, first=False):
        rr = pl.ds(r0, m)
        if first:
            for c in load_rows(1, starts[1], CHUNKS[1]):
                c.start()
            with jax.named_scope("w_bar"):
                pl.semaphore_wait(barrier, 3)
        for group in PAIRS:
            if first:
                with jax.named_scope("w_c0"):
                    for j in group:
                        for c in load_wcat(0, j):
                            c.wait()
            for j in group:
                psend[rr, column(j)] = dot_tb(d[rr, :], wcat[column(j), :]).astype(BF16)
            for j in group:
                to_partner(i, r0, m, j).start()

    def terms(i, r0, m, first=False):
        h = m // 2
        rr, top, bottom = pl.ds(r0, m), pl.ds(r0, h), pl.ds(r0 + h, h)
        for group in PAIRS:
            for j in group:
                if first:
                    with jax.named_scope("w_c1"):
                        for c in load_wcat(1, j):
                            c.wait()
                with jax.named_scope("w_p"):
                    to_partner(i, r0, m, j).wait_recv()
            for j in group:
                v = dot_tb(d[rr, :], wcat[column(chips + j), :]) + precv[rr, column(j)].astype(F32)
                if j == FAR:
                    fsend[rr, :] = v.astype(BF16)
                elif j == RIGHT:
                    nsend[0, bottom, :] = v[h:].astype(BF16)
                    dep[0, pl.ds(0, h), :] = v[:h]
                elif j == LEFT:
                    nsend[1, top, :] = v[:h].astype(BF16)
                    dep[1, pl.ds(0, h), :] = v[h:]
                else:
                    own[lax.rem(i, 2), pl.ds(0, m), :] = v
            if FAR in group:
                for side in range(2):
                    far_copy(i, r0, m, side).start()

    def direct(i, r0, m):
        near_copy(i, r0, m, 0, 1).start()
        near_copy(i, r0, m, 1, 0).start()

    def forward(i, r0, m):
        h = m // 2
        for side in range(2):
            rr = pl.ds(r0 + side * h, h)
            with jax.named_scope('w_f'):
                far_copy(i, r0, m, side).wait_recv()
            nsend[side, rr, :] = (dep[side, pl.ds(0, h), :] + frecv[rr, :].astype(F32)).astype(BF16)
            near_copy(i, r0, m, side, side).start()

    def finish(i, r0, m):
        rr = pl.ds(r0, m)
        for side in range(2):
            for half in range(2):
                with jax.named_scope('w_n'):
                    near_copy(i, r0, m, side, half).wait_recv()
        red[rr, :] = (own[lax.rem(i, 2), pl.ds(0, m), :] + nrecv[0, rr, :].astype(F32) + nrecv[1, rr, :].astype(F32)).astype(BF16)
        write_red(i, r0, m).start()

    half_ff = ff // 2

    def down_copy(q):
        rr = pl.ds(pl.multiple_of(q * half_ff, half_ff), half_ff)
        return pltpu.make_async_copy(down.at[rr], down_hbm.at[rr], down_sem.at[q])

    def down_part(q):
        part = pl.ds(pl.multiple_of(q * half_ff, half_ff), half_ff)
        down[part, :] = product(hid[:, part], dy[:, pl.ds(0, down.shape[1])])
        down_copy(q).start()

    def step(i, r0, m, next_m, last_m, first=False):
        with jax.named_scope("terms"):
            terms(i, r0, m, first)
        if first:
            for k in range(2, steps):
                for c in load_rows(k, starts[k], CHUNKS[k]):
                    c.start()
        if next_m:
            with jax.named_scope("grads"):
                grads(i + 1, r0 + m, next_m)
            direct(i, r0, m)
            with jax.named_scope("exchange"):
                exchange(i + 1, r0 + m, next_m)
            settle(i, r0, m, last_m)
            return

        @pl.loop(0, 2)
        def _(q):
            with jax.named_scope("down"):
                down_part(q)

            @pl.when(q == 0)
            def _():
                for side in range(2):
                    far_copy(i, r0, m, side).wait_send()
                direct(i, r0, m)
                settle(i, r0, m, last_m)

    def settle(i, r0, m, last_m):
        with jax.named_scope("forward"):
            forward(i, r0, m)
        if last_m:
            with jax.named_scope("finish"):
                finish(i - 1, r0 - last_m, last_m)

    with jax.named_scope("grads"):
        grads(0, 0, CHUNKS[0], True)
    with jax.named_scope("exchange"):
        exchange(0, 0, CHUNKS[0], True)
    i = 0
    while i < steps:
        key = (CHUNKS[i], CHUNKS[i + 1] if i + 1 < steps else 0, CHUNKS[i - 1] if i else 0)
        same = 1
        while 0 < i and i + same + 1 < steps and (CHUNKS[i + same], CHUNKS[i + same + 1], CHUNKS[i + same - 1]) == key:
            same += 1
        if same == 1:
            step(i, starts[i], *key, first=i == 0)
        else:
            base, r0, m = i, starts[i], CHUNKS[i]

            @pl.loop(0, same)
            def _(k):
                step(base + k, pl.multiple_of(r0 + k * m, 128), *key)

        i += same
    finish(steps - 1, starts[-1], CHUNKS[-1])
    for q in range(2):
        down_copy(q).wait()

    for i, (r0, m) in enumerate(zip(starts, CHUNKS)):
        for c in write_out(i, r0, m):
            c.wait()
        write_red(i, r0, m).wait()
        for j in range(4):
            to_partner(i, r0, m, j).wait_send()
        for side in range(2):
            if i + 1 < steps:
                far_copy(i, r0, m, side).wait_send()
            for half in range(2):
                near_copy(i, r0, m, side, half).wait_send()


def reduce_terms(n, dy, gate, up, wg, wu, wd):
    rows, width = dy.shape
    ff = gate.shape[1]
    piece = width // n
    steps = len(CHUNKS)
    big = max(CHUNKS)
    half = width // CORES
    dma = pltpu.SemaphoreType.DMA
    any_space = pl.BlockSpec(memory_space=pl.ANY)
    flops = 2 * rows * width * ff * 3
    return pl.pallas_call(
        functools.partial(reduce_kernel, n),
        name="reduce_terms",
        out_shape=[jax.ShapeDtypeStruct((rows, c), BF16) for c in (2 * ff, ff, piece)]
        + [jax.ShapeDtypeStruct((ff, half), BF16)],
        in_specs=[any_space] * 6,
        out_specs=[any_space] * 4,
        scratch_shapes=[
            pltpu.VMEM((width, 2 * ff), BF16),
            pltpu.VMEM((ff, width), BF16),
            pltpu.VMEM((rows, width), BF16),
            pltpu.VMEM((rows, 2 * ff), BF16),
            pltpu.VMEM((rows, ff), BF16),
            pltpu.VMEM((rows, half), BF16),
            pltpu.VMEM((rows, half), BF16),
            pltpu.VMEM((rows, piece), BF16),
            pltpu.VMEM((rows, piece), BF16),
            pltpu.VMEM((2, rows, piece), BF16),
            pltpu.VMEM((2, rows, piece), BF16),
            pltpu.VMEM((2, big // 2, piece), F32),
            pltpu.VMEM((2, big, piece), F32),
            pltpu.VMEM((rows, piece), BF16),
            pltpu.VMEM((ff, half), BF16),
            dma((2, 4, 2)),
            dma((ff // piece,)),
            dma((steps, 3)),
            dma((steps, 2)),
            dma((steps,)),
            dma((2,)),
            dma((steps, 4)),
            dma((steps, 4)),
            dma((steps, 2)),
            dma((steps, 2)),
            dma((steps, 2, 2)),
            dma((steps, 2, 2)),
        ],
        compiler_params=pltpu.CompilerParams(collective_id=0, has_side_effects=True, vmem_limit_bytes=60 * 2**20),
        cost_estimate=pl.CostEstimate(flops=flops, bytes_accessed=60 * 2**20, transcendentals=rows * ff),
    )(dy, gate, up, wg, wu, wd)


def gate_up_kernel(x, d, dw_gate, dw_up):
    @pl.when(pl.program_id(0) == 0)
    def _():
        dw_gate[...] = product(x[...], d[...])

    @pl.when(pl.program_id(0) == 1)
    def _():
        dw_up[...] = product(x[...], d[...])


def gate_up_grads(x, d, bm):
    k, m = x.shape
    ff = d.shape[1] // 2
    last = m // bm - 1
    return pl.pallas_call(
        gate_up_kernel,
        name="gate_up_grads",
        grid=(2, m // bm),
        out_shape=[jax.ShapeDtypeStruct((m, ff), BF16)] * 2,
        in_specs=[pl.BlockSpec((k, bm), lambda j, i: (0, i)), pl.BlockSpec((k, ff), lambda j, i: (0, j))],
        out_specs=[
            pl.BlockSpec((bm, ff), lambda j, i: (i * (1 - j) + last * j, 0)),
            pl.BlockSpec((bm, ff), lambda j, i: (i * j, 0)),
        ],
        compiler_params=pltpu.CompilerParams(vmem_limit_bytes=GATE_UP_VMEM),
        cost_estimate=pl.CostEstimate(flops=4 * k * m * ff, bytes_accessed=2 * (k * m + 2 * (k + m) * ff), transcendentals=0),
    )(x, d)


def own_columns(n, core_hop, chip_hop, width):
    t = lax.axis_index("tp")
    chips = n // CORES
    whose = lax.rem(lax.rem(t, CORES) + core_hop, CORES) * chips + lax.rem(lax.div(t, CORES) + chip_hop, chips)
    return pl.ds(pl.multiple_of(whose * width, width), width)


def piece_copies(n, hops, pieces, dx, held, in_sem, out_sem):
    reads = [pltpu.make_async_copy(p, held.at[q], in_sem.at[q]) for q, p in enumerate(pieces)]
    writes = [
        pltpu.make_async_copy(held.at[q], dx.at[:, own_columns(n, *hop, held.shape[2])], out_sem.at[q])
        for q, hop in enumerate(hops)
    ]
    return reads, writes


def down_kernel(n, hops, hidden_hbm, dy_hbm, part_hbm, *refs):
    count = len(hops)
    pieces = refs[:count]
    dw_down, dx, hidden, dy, out, part, held, load_sem, store_sem, part_sem, in_sem, out_sem = refs[count:]
    tiles, bm, width = out.shape
    ahead = part.shape[1]
    reads, writes = piece_copies(n, hops, pieces, dx, held, in_sem, out_sem)
    def load(q):
        return pltpu.make_async_copy(hidden_hbm.at[:, pl.ds(pl.multiple_of(q * bm, bm), bm)], hidden.at[q], load_sem.at[q])

    def store(q):
        rr = pl.ds(pl.multiple_of(q * bm, bm), bm)
        return pltpu.make_async_copy(out.at[q], dw_down.at[rr, pl.ds(ahead, width)], store_sem.at[q])

    load_dy = pltpu.make_async_copy(dy_hbm.at[:, pl.ds(ahead, width)], dy, load_sem.at[tiles])
    load_part = pltpu.make_async_copy(part_hbm, part, part_sem.at[0])
    store_part = pltpu.make_async_copy(part, dw_down.at[:, pl.ds(0, ahead)], part_sem.at[1])
    load(0).start()
    load_dy.start()
    load(0).wait()
    load_dy.wait()
    for c in [*(load(q) for q in range(1, tiles)), load_part, *reads]:
        c.start()

    @pl.loop(0, tiles)
    def _(q):
        @pl.when(q > 0)
        def _():
            load(q).wait()

        out[q] = product(hidden[q], dy[...])
        store(q).start()

        @pl.when(q == 0)
        def _():
            load_part.wait()
            store_part.start()
            for r, w in zip(reads, writes):
                r.wait()
                w.start()

    for c in [store_part, *(store(q) for q in range(tiles)), *writes]:
        c.wait()


def down_grad(n, hidden, dy, part, hops, pieces, bm):
    k, ff = hidden.shape
    width, ahead = dy.shape[1], part.shape[1]
    rows, piece = pieces[0].shape
    any_space = pl.BlockSpec(memory_space=pl.ANY)
    dma = pltpu.SemaphoreType.DMA
    tiles, rest = ff // bm, width - ahead
    return pl.pallas_call(
        functools.partial(down_kernel, n, hops),
        name="down_grad",
        out_shape=[jax.ShapeDtypeStruct((ff, width), BF16), jax.ShapeDtypeStruct((rows, piece * n), BF16)],
        in_specs=[pl.BlockSpec(memory_space=pltpu.HBM)] * 3 + [any_space] * len(pieces),
        out_specs=[any_space] * 2,
        scratch_shapes=[
            pltpu.VMEM((tiles, k, bm), BF16),
            pltpu.VMEM((k, rest), BF16),
            pltpu.VMEM((tiles, bm, rest), BF16),
            pltpu.VMEM((ff, ahead), BF16),
            pltpu.VMEM((len(pieces), rows, piece), BF16),
            dma((tiles + 1,)),
            dma((tiles,)),
            dma((2,)),
            dma((len(pieces),)),
            dma((len(pieces),)),
        ],
        compiler_params=pltpu.CompilerParams(vmem_limit_bytes=DOWN_VMEM),
        cost_estimate=pl.CostEstimate(flops=2 * k * ff * rest, bytes_accessed=2 * (k * ff + (k + ff) * width), transcendentals=0),
    )(hidden, dy, part, *pieces)


def place_kernel(n, hops, *refs):
    count = len(hops)
    pieces, (dx, sem) = refs[:count], refs[count + 1 :]
    writes = [
        pltpu.make_async_copy(p, dx.at[pl.ds(row, p.shape[0]), own_columns(n, *hop, p.shape[1])], sem.at[q])
        for q, (p, (row, *hop)) in enumerate(zip(pieces, hops))
    ]
    for c in writes:
        c.start()
    for c in writes:
        c.wait()


def place(n, hops, pieces, dx):
    any_space = pl.BlockSpec(memory_space=pl.ANY)
    return pl.pallas_call(
        functools.partial(place_kernel, n, hops),
        name="place",
        out_shape=jax.ShapeDtypeStruct(dx.shape, BF16),
        in_specs=[pl.BlockSpec(memory_space=pltpu.VMEM)] * len(pieces) + [any_space],
        out_specs=any_space,
        input_output_aliases={len(pieces): 0},
        scratch_shapes=[pltpu.SemaphoreType.DMA((len(pieces),))],
        compiler_params=pltpu.CompilerParams(vmem_limit_bytes=16 * 2**20),
        cost_estimate=pl.CostEstimate(flops=0, bytes_accessed=sum(4 * p.size for p in pieces), transcendentals=0),
    )(*pieces, dx)


def solution(mesh):
    n = mesh.shape["tp"]
    to_right = [(i, (i + CORES) % n) for i in range(n)]
    to_left = [(i, (i - CORES) % n) for i in range(n)]
    swap = [(i, i ^ 1) for i in range(n)]

    def send(v, where):
        return lax.ppermute(v, "tp", where)

    def step(x, dy, gate, up, w_gate, w_up, w_down):
        d, hidden, red, part = reduce_terms(n, dy, gate, up, w_gate, w_up, w_down)
        h = red.shape[0] // 2
        chips = n // CORES
        from_left, from_right, other = send(red, to_right), send(red, to_left), send(red, swap)
        dw_gate, dw_up = gate_up_grads(*(pltpu.with_memory_space_constraint(v, pltpu.HBM) for v in (x, d)), 1024)
        from_left, from_right, other, dw_gate, dw_up, hidden = lax.optimization_barrier(
            (from_left, from_right, other, dw_gate, dw_up, hidden)
        )
        far = send(from_left[:h], to_right), send(from_right[h:], to_left)
        left2, right2 = send(from_left, swap), send(from_right, swap)
        dw_down, dx = down_grad(
            n, hidden, dy, part, ((0, 0), (1, 0), (0, chips - 1), (0, 1)), (red, other, from_left, from_right), 512
        )
        left2, right2, dw_down, dx = lax.optimization_barrier((left2, right2, dw_down, dx))
        dx = place(n, ((0, 1, chips - 1), (0, 1, 1)), (left2, right2), dx)
        far, dx = lax.optimization_barrier((far, dx))
        far2 = [send(v, swap) for v in far]
        dx = place(n, ((0, 0, 2), (h, 0, 2), (0, 1, 2), (h, 1, 2)), (*far, *far2), dx)
        return dx, dw_gate, dw_up, dw_down

    tokens, columns, rows = P("dp", None), P(None, "tp"), P("tp", None)
    return jax.shard_map(
        step,
        mesh=mesh,
        in_specs=(tokens, tokens, P("dp", "tp"), P("dp", "tp"), columns, columns, rows),
        out_specs=(tokens, P("dp", "tp"), P("dp", "tp"), P(("dp", "tp"), None)),
        check_vma=False,
    )
```

```python
import functools

import jax
import jax.numpy as jnp
from jax import lax
from jax.experimental import pallas as pl
from jax.experimental.pallas import tpu as pltpu
from jax.sharding import PartitionSpec as P


BF16, F32 = jnp.bfloat16, jnp.float32
CONTRACT_LAST = (((1,), (1,)), ((), ()))
CONTRACT_FIRST = (((0,), (0,)), ((), ()))
CORES = 2
GATE_UP_VMEM, DOWN_VMEM = 36 * 2**20, 40 * 2**20
CHUNKS = (256, 384, 384, 384, 384, 256)
FAR, RIGHT, LEFT, OWN = range(4)
PAIRS = ((FAR, RIGHT), (LEFT, OWN))


def dot_tb(a, b):
    return lax.dot_general(a, b, CONTRACT_LAST, preferred_element_type=F32)


def product(a, b):
    return lax.dot_general(a, b, CONTRACT_FIRST, preferred_element_type=F32).astype(BF16)


def reduce_kernel(
    n, dy_hbm, gate_hbm, up_hbm, wg_hbm, wu_hbm, wd_hbm, d_hbm, hid_hbm, red_hbm, down_hbm,
    wcat, wd, dy, d, hid, psend, precv, fsend, frecv, nsend, nrecv, dep, own, red, down,
    wcat_sem, wd_sem, in_sem, out_sem, red_sem, down_sem, p_ssem, p_rsem, f_ssem, f_rsem, n_ssem, n_rsem,
):
    rows, width = dy.shape
    ff = wd.shape[0]
    piece = width // n
    chips = n // CORES
    steps = len(CHUNKS)

    t = lax.axis_index("tp")
    chip, core = lax.div(t, CORES), lax.rem(t, CORES)
    partner = t + 1 - 2 * core
    right, left = lax.rem(t + CORES, n), lax.rem(t + n - CORES, n)
    owner = [lax.rem(chip + hop, chips) for hop in (2, 1, chips - 1, 0)]

    def load_rows(i, r0, m):
        rr = pl.ds(r0, m)
        return [
            pltpu.make_async_copy(dy_hbm.at[rr], dy.at[rr], in_sem.at[i, 0]),
            pltpu.make_async_copy(gate_hbm.at[rr], d.at[rr, pl.ds(0, ff)], in_sem.at[i, 1]),
            pltpu.make_async_copy(up_hbm.at[rr], d.at[rr, pl.ds(ff, ff)], in_sem.at[i, 2]),
        ]

    blocks = ff // piece

    def load_wd(b):
        rr = pl.ds(b * piece, piece)
        return pltpu.make_async_copy(wd_hbm.at[rr], wd.at[rr], wd_sem.at[b])

    def load_wcat(half, j):
        whose = lax.rem(core + 1 + half, CORES)
        src = pl.ds(pl.multiple_of((whose * chips + owner[j]) * piece, piece), piece)
        dst = pl.ds((half * chips + j) * piece, piece)
        return [
            pltpu.make_async_copy(w.at[src], wcat.at[dst, pl.ds(k * ff, ff)], wcat_sem.at[half, j, k])
            for k, w in enumerate((wg_hbm, wu_hbm))
        ]

    def load_half(half):
        for j in range(4):
            for c in load_wcat(half, j):
                c.start()

    starts = [sum(CHUNKS[:i]) for i in range(steps)]
    for c in load_rows(0, starts[0], CHUNKS[0]):
        c.start()
    for b in range(blocks):
        load_wd(b).start()

    barrier = pltpu.get_barrier_semaphore()
    for other in (partner, left, right):
        pl.semaphore_signal(barrier, inc=1, device_id={"tp": other})

    def column(j):
        return pl.ds(j * piece, piece)

    def to_partner(i, r0, m, j):
        rr = pl.ds(r0, m)
        return pltpu.make_async_remote_copy(
            psend.at[rr, column(j)], precv.at[rr, column(j)], p_ssem.at[i, j], p_rsem.at[i, j], device_id={"tp": partner}
        )

    def far_copy(i, r0, m, side):
        rr = pl.ds(r0 + side * (m // 2), m // 2)
        return pltpu.make_async_remote_copy(
            fsend.at[rr], frecv.at[rr], f_ssem.at[i, side], f_rsem.at[i, side], device_id={"tp": (right, left)[side]}
        )

    def near_copy(i, r0, m, side, half):
        rr = pl.ds(r0 + half * (m // 2), m // 2)
        return pltpu.make_async_remote_copy(
            nsend.at[side, rr], nrecv.at[side, rr], n_ssem.at[i, side, half], n_rsem.at[i, side, half],
            device_id={"tp": (right, left)[side]},
        )

    def write_out(i, r0, m):
        rr = pl.ds(r0, m)
        return [
            pltpu.make_async_copy(d.at[rr], d_hbm.at[rr], out_sem.at[i, 0]),
            pltpu.make_async_copy(hid.at[rr], hid_hbm.at[rr], out_sem.at[i, 1]),
        ]

    def write_red(i, r0, m):
        rr = pl.ds(r0, m)
        return pltpu.make_async_copy(red.at[rr], red_hbm.at[rr], red_sem.at[i])

    def grads(i, r0, m, first=False):
        rr = pl.ds(r0, m)
        with jax.named_scope("w_in"):
            for c in load_rows(i, r0, m):
                c.wait()
        if first:
            load_half(0)
            with jax.named_scope("w_wd"):
                for b in range(blocks):
                    load_wd(b).wait()
            load_half(1)
        for b in range(blocks):
            cg, cu = column(b), pl.ds(ff + b * piece, piece)
            dh = dot_tb(dy[rr, :], wd[column(b), :])
            g, u = d[rr, cg].astype(F32), d[rr, cu].astype(F32)
            s = jax.nn.sigmoid(g)
            silu = g * s
            hid[rr, cg] = (silu * u).astype(BF16)
            d[rr, cg] = (dh * u * (s + silu * (1.0 - s))).astype(BF16)
            d[rr, cu] = (dh * silu).astype(BF16)
        for c in write_out(i, r0, m):
            c.start()

    def exchange(i, r0, m, first=False):
        rr = pl.ds(r0, m)
        if first:
            for c in load_rows(1, starts[1], CHUNKS[1]):
                c.start()
            with jax.named_scope("w_bar"):
                pl.semaphore_wait(barrier, 3)
        for group in PAIRS:
            if first:
                with jax.named_scope("w_c0"):
                    for j in group:
                        for c in load_wcat(0, j):
                            c.wait()
            for j in group:
                psend[rr, column(j)] = dot_tb(d[rr, :], wcat[column(j), :]).astype(BF16)
            for j in group:
                to_partner(i, r0, m, j).start()

    def terms(i, r0, m, first=False):
        h = m // 2
        rr, top, bottom = pl.ds(r0, m), pl.ds(r0, h), pl.ds(r0 + h, h)
        for group in PAIRS:
            for j in group:
                if first:
                    with jax.named_scope("w_c1"):
                        for c in load_wcat(1, j):
                            c.wait()
                with jax.named_scope("w_p"):
                    to_partner(i, r0, m, j).wait_recv()
            for j in group:
                v = dot_tb(d[rr, :], wcat[column(chips + j), :]) + precv[rr, column(j)].astype(F32)
                if j == FAR:
                    fsend[rr, :] = v.astype(BF16)
                elif j == RIGHT:
                    nsend[0, bottom, :] = v[h:].astype(BF16)
                    dep[0, pl.ds(0, h), :] = v[:h]
                elif j == LEFT:
                    nsend[1, top, :] = v[:h].astype(BF16)
                    dep[1, pl.ds(0, h), :] = v[h:]
                else:
                    own[lax.rem(i, 2), pl.ds(0, m), :] = v
            if FAR in group:
                for side in range(2):
                    far_copy(i, r0, m, side).start()

    def direct(i, r0, m):
        near_copy(i, r0, m, 0, 1).start()
        near_copy(i, r0, m, 1, 0).start()

    def forward(i, r0, m):
        h = m // 2
        for side in range(2):
            rr = pl.ds(r0 + side * h, h)
            with jax.named_scope('w_f'):
                far_copy(i, r0, m, side).wait_recv()
            nsend[side, rr, :] = (dep[side, pl.ds(0, h), :] + frecv[rr, :].astype(F32)).astype(BF16)
            near_copy(i, r0, m, side, side).start()

    def finish(i, r0, m):
        rr = pl.ds(r0, m)
        for side in range(2):
            for half in range(2):
                with jax.named_scope('w_n'):
                    near_copy(i, r0, m, side, half).wait_recv()
        red[rr, :] = (own[lax.rem(i, 2), pl.ds(0, m), :] + nrecv[0, rr, :].astype(F32) + nrecv[1, rr, :].astype(F32)).astype(BF16)
        write_red(i, r0, m).start()

    half_ff = ff // 2

    def down_copy(q):
        rr = pl.ds(pl.multiple_of(q * half_ff, half_ff), half_ff)
        return pltpu.make_async_copy(down.at[rr], down_hbm.at[rr], down_sem.at[q])

    def down_part(q):
        part = pl.ds(pl.multiple_of(q * half_ff, half_ff), half_ff)
        down[part, :] = product(hid[:, part], dy[:, pl.ds(0, down.shape[1])])
        down_copy(q).start()

    def step(i, r0, m, next_m, last_m, first=False):
        with jax.named_scope("terms"):
            terms(i, r0, m, first)
        if first:
            for k in range(2, steps):
                for c in load_rows(k, starts[k], CHUNKS[k]):
                    c.start()
        if next_m:
            with jax.named_scope("grads"):
                grads(i + 1, r0 + m, next_m)
            direct(i, r0, m)
            with jax.named_scope("exchange"):
                exchange(i + 1, r0 + m, next_m)
            settle(i, r0, m, last_m)
            return

        @pl.loop(0, 2)
        def _(q):
            with jax.named_scope("down"):
                down_part(q)

            @pl.when(q == 0)
            def _():
                for side in range(2):
                    far_copy(i, r0, m, side).wait_send()
                direct(i, r0, m)
                settle(i, r0, m, last_m)

    def settle(i, r0, m, last_m):
        with jax.named_scope("forward"):
            forward(i, r0, m)
        if last_m:
            with jax.named_scope("finish"):
                finish(i - 1, r0 - last_m, last_m)

    with jax.named_scope("grads"):
        grads(0, 0, CHUNKS[0], True)
    with jax.named_scope("exchange"):
        exchange(0, 0, CHUNKS[0], True)
    i = 0
    while i < steps:
        key = (CHUNKS[i], CHUNKS[i + 1] if i + 1 < steps else 0, CHUNKS[i - 1] if i else 0)
        same = 1
        while 0 < i and i + same + 1 < steps and (CHUNKS[i + same], CHUNKS[i + same + 1], CHUNKS[i + same - 1]) == key:
            same += 1
        if same == 1:
            step(i, starts[i], *key, first=i == 0)
        else:
            base, r0, m = i, starts[i], CHUNKS[i]

            @pl.loop(0, same)
            def _(k):
                step(base + k, pl.multiple_of(r0 + k * m, 128), *key)

        i += same
    finish(steps - 1, starts[-1], CHUNKS[-1])
    for q in range(2):
        down_copy(q).wait()

    for i, (r0, m) in enumerate(zip(starts, CHUNKS)):
        for c in write_out(i, r0, m):
            c.wait()
        write_red(i, r0, m).wait()
        for j in range(4):
            to_partner(i, r0, m, j).wait_send()
        for side in range(2):
            if i + 1 < steps:
                far_copy(i, r0, m, side).wait_send()
            for half in range(2):
                near_copy(i, r0, m, side, half).wait_send()


def reduce_terms(n, dy, gate, up, wg, wu, wd):
    rows, width = dy.shape
    ff = gate.shape[1]
    piece = width // n
    steps = len(CHUNKS)
    big = max(CHUNKS)
    half = width // CORES
    dma = pltpu.SemaphoreType.DMA
    any_space = pl.BlockSpec(memory_space=pl.ANY)
    flops = 2 * rows * width * ff * 3
    return pl.pallas_call(
        functools.partial(reduce_kernel, n),
        name="reduce_terms",
        out_shape=[jax.ShapeDtypeStruct((rows, c), BF16) for c in (2 * ff, ff, piece)]
        + [jax.ShapeDtypeStruct((ff, half), BF16)],
        in_specs=[any_space] * 6,
        out_specs=[any_space] * 4,
        scratch_shapes=[
            pltpu.VMEM((width, 2 * ff), BF16),
            pltpu.VMEM((ff, width), BF16),
            pltpu.VMEM((rows, width), BF16),
            pltpu.VMEM((rows, 2 * ff), BF16),
            pltpu.VMEM((rows, ff), BF16),
            pltpu.VMEM((rows, half), BF16),
            pltpu.VMEM((rows, half), BF16),
            pltpu.VMEM((rows, piece), BF16),
            pltpu.VMEM((rows, piece), BF16),
            pltpu.VMEM((2, rows, piece), BF16),
            pltpu.VMEM((2, rows, piece), BF16),
            pltpu.VMEM((2, big // 2, piece), F32),
            pltpu.VMEM((2, big, piece), F32),
            pltpu.VMEM((rows, piece), BF16),
            pltpu.VMEM((ff, half), BF16),
            dma((2, 4, 2)),
            dma((ff // piece,)),
            dma((steps, 3)),
            dma((steps, 2)),
            dma((steps,)),
            dma((2,)),
            dma((steps, 4)),
            dma((steps, 4)),
            dma((steps, 2)),
            dma((steps, 2)),
            dma((steps, 2, 2)),
            dma((steps, 2, 2)),
        ],
        compiler_params=pltpu.CompilerParams(collective_id=0, has_side_effects=True, vmem_limit_bytes=60 * 2**20),
        cost_estimate=pl.CostEstimate(flops=flops, bytes_accessed=60 * 2**20, transcendentals=rows * ff),
    )(dy, gate, up, wg, wu, wd)


def gate_up_kernel(x, d, dw_gate, dw_up):
    @pl.when(pl.program_id(0) == 0)
    def _():
        dw_gate[...] = product(x[...], d[...])

    @pl.when(pl.program_id(0) == 1)
    def _():
        dw_up[...] = product(x[...], d[...])


def gate_up_grads(x, d, bm):
    k, m = x.shape
    ff = d.shape[1] // 2
    last = m // bm - 1
    return pl.pallas_call(
        gate_up_kernel,
        name="gate_up_grads",
        grid=(2, m // bm),
        out_shape=[jax.ShapeDtypeStruct((m, ff), BF16)] * 2,
        in_specs=[pl.BlockSpec((k, bm), lambda j, i: (0, i)), pl.BlockSpec((k, ff), lambda j, i: (0, j))],
        out_specs=[
            pl.BlockSpec((bm, ff), lambda j, i: (i * (1 - j) + last * j, 0)),
            pl.BlockSpec((bm, ff), lambda j, i: (i * j, 0)),
        ],
        compiler_params=pltpu.CompilerParams(vmem_limit_bytes=GATE_UP_VMEM),
        cost_estimate=pl.CostEstimate(flops=4 * k * m * ff, bytes_accessed=2 * (k * m + 2 * (k + m) * ff), transcendentals=0),
    )(x, d)


def own_columns(n, core_hop, chip_hop, width):
    t = lax.axis_index("tp")
    chips = n // CORES
    whose = lax.rem(lax.rem(t, CORES) + core_hop, CORES) * chips + lax.rem(lax.div(t, CORES) + chip_hop, chips)
    return pl.ds(pl.multiple_of(whose * width, width), width)


def piece_copies(n, hops, pieces, dx, held, in_sem, out_sem):
    reads = [pltpu.make_async_copy(p, held.at[q], in_sem.at[q]) for q, p in enumerate(pieces)]
    writes = [
        pltpu.make_async_copy(held.at[q], dx.at[:, own_columns(n, *hop, held.shape[2])], out_sem.at[q])
        for q, hop in enumerate(hops)
    ]
    return reads, writes


def down_kernel(n, hops, hidden_hbm, dy_hbm, part_hbm, *refs):
    count = len(hops)
    pieces = refs[:count]
    dw_down, dx, hidden, dy, out, part, held, load_sem, store_sem, part_sem, in_sem, out_sem = refs[count:]
    tiles, bm, width = out.shape
    ahead = part.shape[1]
    reads, writes = piece_copies(n, hops, pieces, dx, held, in_sem, out_sem)
    def load(q):
        return pltpu.make_async_copy(hidden_hbm.at[:, pl.ds(pl.multiple_of(q * bm, bm), bm)], hidden.at[q], load_sem.at[q])

    def store(q):
        rr = pl.ds(pl.multiple_of(q * bm, bm), bm)
        return pltpu.make_async_copy(out.at[q], dw_down.at[rr, pl.ds(ahead, width)], store_sem.at[q])

    load_dy = pltpu.make_async_copy(dy_hbm.at[:, pl.ds(ahead, width)], dy, load_sem.at[tiles])
    load_part = pltpu.make_async_copy(part_hbm, part, part_sem.at[0])
    store_part = pltpu.make_async_copy(part, dw_down.at[:, pl.ds(0, ahead)], part_sem.at[1])
    load(0).start()
    load_dy.start()
    load(0).wait()
    load_dy.wait()
    for c in [*(load(q) for q in range(1, tiles)), load_part, *reads]:
        c.start()

    @pl.loop(0, tiles)
    def _(q):
        @pl.when(q > 0)
        def _():
            load(q).wait()

        out[q] = product(hidden[q], dy[...])
        store(q).start()

        @pl.when(q == 0)
        def _():
            load_part.wait()
            store_part.start()
            for r, w in zip(reads, writes):
                r.wait()
                w.start()

    for c in [store_part, *(store(q) for q in range(tiles)), *writes]:
        c.wait()


def down_grad(n, hidden, dy, part, hops, pieces, bm):
    k, ff = hidden.shape
    width, ahead = dy.shape[1], part.shape[1]
    rows, piece = pieces[0].shape
    any_space = pl.BlockSpec(memory_space=pl.ANY)
    dma = pltpu.SemaphoreType.DMA
    tiles, rest = ff // bm, width - ahead
    return pl.pallas_call(
        functools.partial(down_kernel, n, hops),
        name="down_grad",
        out_shape=[jax.ShapeDtypeStruct((ff, width), BF16), jax.ShapeDtypeStruct((rows, piece * n), BF16)],
        in_specs=[pl.BlockSpec(memory_space=pltpu.HBM)] * 3 + [any_space] * len(pieces),
        out_specs=[any_space] * 2,
        scratch_shapes=[
            pltpu.VMEM((tiles, k, bm), BF16),
            pltpu.VMEM((k, rest), BF16),
            pltpu.VMEM((tiles, bm, rest), BF16),
            pltpu.VMEM((ff, ahead), BF16),
            pltpu.VMEM((len(pieces), rows, piece), BF16),
            dma((tiles + 1,)),
            dma((tiles,)),
            dma((2,)),
            dma((len(pieces),)),
            dma((len(pieces),)),
        ],
        compiler_params=pltpu.CompilerParams(vmem_limit_bytes=DOWN_VMEM),
        cost_estimate=pl.CostEstimate(flops=2 * k * ff * rest, bytes_accessed=2 * (k * ff + (k + ff) * width), transcendentals=0),
    )(hidden, dy, part, *pieces)


def place_kernel(n, hops, *refs):
    count = len(hops)
    pieces, (dx, sem) = refs[:count], refs[count + 1 :]
    writes = [
        pltpu.make_async_copy(p, dx.at[pl.ds(row, p.shape[0]), own_columns(n, *hop, p.shape[1])], sem.at[q])
        for q, (p, (row, *hop)) in enumerate(zip(pieces, hops))
    ]
    for c in writes:
        c.start()
    for c in writes:
        c.wait()


def place(n, hops, pieces, dx):
    any_space = pl.BlockSpec(memory_space=pl.ANY)
    return pl.pallas_call(
        functools.partial(place_kernel, n, hops),
        name="place",
        out_shape=jax.ShapeDtypeStruct(dx.shape, BF16),
        in_specs=[pl.BlockSpec(memory_space=pltpu.VMEM)] * len(pieces) + [any_space],
        out_specs=any_space,
        input_output_aliases={len(pieces): 0},
        scratch_shapes=[pltpu.SemaphoreType.DMA((len(pieces),))],
        compiler_params=pltpu.CompilerParams(vmem_limit_bytes=16 * 2**20),
        cost_estimate=pl.CostEstimate(flops=0, bytes_accessed=sum(4 * p.size for p in pieces), transcendentals=0),
    )(*pieces, dx)


def solution(mesh):
    n = mesh.shape["tp"]
    to_right = [(i, (i + CORES) % n) for i in range(n)]
    to_left = [(i, (i - CORES) % n) for i in range(n)]
    swap = [(i, i ^ 1) for i in range(n)]

    def send(v, where):
        return lax.ppermute(v, "tp", where)

    def step(x, dy, gate, up, w_gate, w_up, w_down):
        d, hidden, red, part = reduce_terms(n, dy, gate, up, w_gate, w_up, w_down)
        h = red.shape[0] // 2
        chips = n // CORES
        from_left, from_right, other = send(red, to_right), send(red, to_left), send(red, swap)
        dw_gate, dw_up = gate_up_grads(*(pltpu.with_memory_space_constraint(v, pltpu.HBM) for v in (x, d)), 512)
        from_left, from_right, other, dw_gate, dw_up, hidden = lax.optimization_barrier(
            (from_left, from_right, other, dw_gate, dw_up, hidden)
        )
        far = send(from_left[:h], to_right), send(from_right[h:], to_left)
        left2, right2 = send(from_left, swap), send(from_right, swap)
        dw_down, dx = down_grad(
            n, hidden, dy, part, ((0, 0), (1, 0), (0, chips - 1), (0, 1)), (red, other, from_left, from_right), 512
        )
        left2, right2, dw_down, dx = lax.optimization_barrier((left2, right2, dw_down, dx))
        dx = place(n, ((0, 1, chips - 1), (0, 1, 1)), (left2, right2), dx)
        far, dx = lax.optimization_barrier((far, dx))
        far2 = [send(v, swap) for v in far]
        dx = place(n, ((0, 0, 2), (h, 0, 2), (0, 1, 2), (h, 1, 2)), (*far, *far2), dx)
        return dx, dw_gate, dw_up, dw_down

    tokens, columns, rows = P("dp", None), P(None, "tp"), P("tp", None)
    return jax.shard_map(
        step,
        mesh=mesh,
        in_specs=(tokens, tokens, P("dp", "tp"), P("dp", "tp"), columns, columns, rows),
        out_specs=(tokens, P("dp", "tp"), P("dp", "tp"), P(("dp", "tp"), None)),
        check_vma=False,
    )
```
